32 devices in a mesh: ens: 4 (over y, x), lat: 2 (over core), lon: 4 (over z).
Axes of the slice: x: 2, y: 2, z: 4, core: 2. Of those that a mesh axis runs over, the one named last changes fastest.
Arguments:
- fields: bfloat16 [8, 36, 96, 384], P('ens', 'lat', 'lon'), parts along dimension 0, may hold values from -6 to 6
- region_ids: int32 [2, 36, 96], P(None, 'lat', 'lon'), may hold values from 0 to 3
- bias_index: int32 [144, 144], replicated, may hold values from 0 to 3311
- earth_bias: bfloat16 [6, 3312, 12], P('lat'), may hold values from -70 to 170
- w_qkv: bfloat16 [384, 1152], replicated, may hold values from -0.3125 to 0.3125
- w_proj: bfloat16 [384, 384], replicated, may hold values from -0.3125 to 0.3125
- w_fc1: bfloat16 [384, 1536], replicated, may hold values from -0.3125 to 0.3125
- w_fc2: bfloat16 [1536, 384], replicated, may hold values from -0.15625 to 0.15625
Outputs:
- result: bfloat16 [8, 36, 96, 384], P('ens', 'lat', 'lon'), parts along dimension 0
The draws below stay inside these ranges and needn't reach their ends.
There are 4 independent parts, one for each index of `ens`. The reference program is written for one: setup_inputs(seed, part) draws one part's arguments, and reference() takes and returns one part's arrays. A program takes and returns all parts, laid end to end along the dimension named above; an argument that names none is the same for every part. Nothing has to cross between parts.
All inputs are finite; a program needn't handle non-finite values.
Results may differ from the reference program's by a relative error of at most 0.009.
Values may be sent and summed in bfloat16 or wider, within the bound.
A program may use at most 128 MiB of HBM per device.

```python
import jax
import jax.numpy as jnp
from jax import lax

C = 384
HEADS = 12
FFH = 1536
WZ = 2
WLAT = 6
WLON = 12
LEV = 2
WIN_TOK = 144
BIAS_POS = 3312
NLAT = 36
NLON = 96
LATW = 6


def draw_earth_bias(key, part):
    key_base, key_offset = jax.random.split(jax.random.fold_in(key, 17))
    table_shape = (LATW, BIAS_POS, HEADS)
    values = jnp.clip(jax.random.normal(key_base, table_shape, jnp.float32), -4.0, 4.0)
    return values.astype(jnp.bfloat16)


def with_ends(drawn, rng, low, largest):
    spot = [jax.random.randint(jax.random.fold_in(rng, axis), (), 0, length) for axis, length in enumerate(drawn.shape)]
    widest = drawn.shape.index(max(drawn.shape))
    beside = spot[:widest] + [(spot[widest] + 1) % drawn.shape[widest]] + spot[widest + 1:]
    return drawn.at[tuple(spot)].set(low).at[tuple(beside)].set(largest)


def block_scale(rng, extent, pieces, smallest, largest):
    def one(axis_at, shards_of):
        steps = jax.random.uniform(jax.random.fold_in(jax.random.fold_in(rng, 6), axis_at), (shards_of,), jnp.float32, smallest / len(pieces), largest / len(pieces))
        return jnp.repeat(jnp.exp(steps), extent[axis_at] // shards_of).reshape((-1,) + (1,) * (len(extent) - axis_at - 1))

    gain = one(*pieces[0])
    for cut in pieces[1:]:
        gain = gain * one(*cut)
    return gain


def normal_values(stream_key, extent, scale, reach, cuts=(), dtype=jnp.bfloat16):
    drawn = jax.random.normal(stream_key, extent, jnp.float32) * scale
    if len(cuts) > 0:
        drawn = block_scale(stream_key, extent, cuts, -0.22, 0.18) * drawn
    return jnp.clip(drawn, min=-reach, max=reach).astype(dtype)


def setup_inputs(seed: int = 0, part: int = 0) -> dict:
    arg_keys = jax.random.split(jax.random.key(seed), 9)
    part_keys = jax.random.split(jax.random.fold_in(arg_keys[8], part), 9)
    fields = normal_values(part_keys[0], (LEV, NLAT, NLON, C), 1.0, 6.0, ((1, 2), (2, 4)))
    region_ids = with_ends(jax.random.randint(arg_keys[1], (LEV, NLAT, NLON), 0, 4), jax.random.fold_in(arg_keys[1], 1), 0, 3).astype(jnp.int32)
    bias_index = with_ends(jax.random.randint(arg_keys[2], (WIN_TOK, WIN_TOK), 0, BIAS_POS), jax.random.fold_in(arg_keys[2], 1), 0, BIAS_POS - 1).astype(jnp.int32)
    earth_bias = draw_earth_bias(jax.random.fold_in(arg_keys[8], 71), part)
    w_qkv = normal_values(arg_keys[4], (C, 3 * C), C ** -0.5, 0.3125)
    w_proj = normal_values(arg_keys[5], (C, C), C ** -0.5, 0.3125)
    w_fc1 = normal_values(arg_keys[6], (C, FFH), C ** -0.5, 0.3125)
    w_fc2 = normal_values(arg_keys[7], (FFH, C), FFH ** -0.5, 0.15625)
    return {"fields": fields, "region_ids": region_ids, "bias_index": bias_index, "earth_bias": earth_bias, "w_qkv": w_qkv, "w_proj": w_proj, "w_fc1": w_fc1, "w_fc2": w_fc2}


EPS_NORM = 1e-05

def layer_norm(tokens_in):
    widened = tokens_in.astype(jnp.float32)
    average = lax.optimization_barrier(jnp.mean(widened, axis=-1, keepdims=True))
    centred = widened - average
    spread = lax.optimization_barrier(jnp.mean(centred * centred, axis=-1, keepdims=True))
    return (centred * lax.rsqrt(spread + EPS_NORM)).astype(jnp.bfloat16)

def attend(normed, region_block, bias_block, bias_index, w_qkv, w_proj):
    levels, lat_rows, lon_cols, feature_width = normed.shape
    lat_wins = lat_rows // WLAT
    lon_wins = lon_cols // WLON
    window_tokens = levels * WLAT * WLON
    head_count = bias_block.shape[-1]
    head_dim = feature_width // head_count
    windowed = normed.reshape(levels, lat_wins, WLAT, lon_wins, WLON, feature_width)
    windowed = windowed.transpose(1, 3, 0, 2, 4, 5).reshape(-1, feature_width)
    packed = jnp.dot(windowed, w_qkv, preferred_element_type=jnp.float32).astype(jnp.bfloat16)
    packed = packed.reshape(lat_wins, lon_wins, window_tokens, 3, head_count, head_dim)
    queries = packed[:, :, :, 0].astype(jnp.float32)
    key_rows = packed[:, :, :, 1].astype(jnp.float32)
    value_rows = packed[:, :, :, 2].astype(jnp.float32)
    regions = region_block.reshape(levels, lat_wins, WLAT, lon_wins, WLON)
    regions = regions.transpose(1, 3, 0, 2, 4).reshape(lat_wins, lon_wins, window_tokens)
    bias_table = bias_block[:, bias_index, :].astype(jnp.float32).transpose(0, 3, 1, 2)
    scores = jnp.einsum('abihd,abjhd->abhij', queries, key_rows) * head_dim ** (-0.5) + bias_table[:, None]
    allowed = regions[:, :, :, None] == regions[:, :, None, :]
    scores = jnp.where(allowed[:, :, None], scores, -jnp.inf)
    maxima = lax.optimization_barrier(jnp.max(scores, axis=-1, keepdims=True))
    exponent = jnp.exp(scores - maxima)
    attn_weights = (exponent / lax.optimization_barrier(jnp.sum(exponent, axis=-1, keepdims=True))).astype(jnp.bfloat16)
    context = jnp.einsum('abhij,abjhd->abihd', attn_weights.astype(jnp.float32), value_rows)
    context = context.astype(jnp.bfloat16).reshape(-1, feature_width)
    projected = jnp.dot(context, w_proj, preferred_element_type=jnp.float32).astype(jnp.bfloat16)
    projected = projected.reshape(lat_wins, lon_wins, levels, WLAT, WLON, feature_width)
    return projected.transpose(2, 0, 3, 1, 4, 5).reshape(levels, lat_rows, lon_cols, feature_width)

def feed_forward(residual, w_fc1, w_fc2):
    feature_width = residual.shape[-1]
    normed = layer_norm(residual).reshape(-1, feature_width)
    hidden = jax.nn.gelu(jnp.dot(normed, w_fc1, preferred_element_type=jnp.float32), approximate=False)
    hidden = hidden.astype(jnp.bfloat16)
    summed = residual.reshape(-1, feature_width).astype(jnp.float32) + jnp.dot(hidden, w_fc2, preferred_element_type=jnp.float32)
    return summed.astype(jnp.bfloat16).reshape(residual.shape)

def reference(fields, region_ids, bias_index, earth_bias, w_qkv, w_proj, w_fc1, w_fc2):
    half_lev = WZ // 2
    half_lat = WLAT // 2
    half_lon = WLON // 2
    normed = layer_norm(fields)
    shifted = jnp.roll(normed, (-half_lev, -half_lat, -half_lon), axis=(0, 1, 2))
    blocks = shifted.reshape(LEV, LATW, WLAT, NLON, C).transpose(1, 0, 2, 3, 4)
    region_blocks = region_ids.reshape(LEV, LATW, WLAT, NLON).transpose(1, 0, 2, 3)

    def one_band(packed_in):
        lat_band, regions, bias_table = packed_in
        return attend(lat_band, regions, bias_table[None], bias_index, w_qkv, w_proj)
    outputs = lax.map(one_band, (blocks, region_blocks, earth_bias))
    attn_out = outputs.transpose(1, 0, 2, 3, 4).reshape(LEV, NLAT, NLON, C)
    returned = jnp.roll(attn_out, (half_lev, half_lat, half_lon), axis=(0, 1, 2))
    residual = (fields.astype(jnp.float32) + returned.astype(jnp.float32)).astype(jnp.bfloat16)
    return feed_forward(residual, w_fc1, w_fc2)
```

```python
import functools
import math

import jax
import jax.numpy as jnp
from jax import lax
from jax.experimental import pallas as pl
from jax.experimental.pallas import tpu as pltpu
from jax.sharding import PartitionSpec as P

WZ = 2
WLAT = 6
WLON = 12
HALF_LAT = WLAT // 2
HALF_LON = WLON // 2
EPS_NORM = 1e-05
LOG2E = math.log2(math.e)
LO = 256
LANES = 128
AT_ONCE = 4
GRANT = 48 * 1024 * 1024
NT = (((1,), (1,)), ((), ()))
MESH = pl.DeviceIdType.MESH


def norm_rows(wide):
    average = jnp.mean(wide, axis=-1, keepdims=True)
    centred = wide - average
    spread = jnp.mean(centred * centred, axis=-1, keepdims=True)
    return (centred * lax.rsqrt(spread + EPS_NORM)).astype(jnp.bfloat16)


def build_table(earth, table, slab):
    bands, positions, heads = earth.shape
    for piece in range(table.shape[0] // slab):
        start = piece * LO
        size = min(LO, positions - start)
        parts = [earth[band, start : start + size, :].astype(jnp.float32) for band in range(bands)]
        wide = jnp.concatenate(parts, axis=1)
        wide = jnp.pad(wide, ((0, LO - size), (0, LANES - wide.shape[1])))
        table[piece * slab : (piece + 1) * slab, :] = wide.T[:slab].astype(jnp.bfloat16)


def fill_bias(main_idx, rest_idx, table, bias, slab, step):
    tokens = main_idx.shape[0]
    rest = rest_idx.shape[0]
    pieces = table.shape[0] // slab
    low = lax.broadcasted_iota(jnp.int32, (LO, LANES), 0)

    def lookup(lines):
        spots = [jnp.where(low == (row & (LO - 1)), 1.0, 0.0).astype(jnp.bfloat16) for row in lines]
        found = jnp.dot(
            table[...], jnp.concatenate(spots, axis=1), preferred_element_type=jnp.float32
        )
        picked = []
        for place, row in enumerate(lines):
            high = row // LO
            columns = found[:, place * LANES : (place + 1) * LANES]
            total = columns[(pieces - 1) * slab :]
            for piece in range(pieces - 1):
                total = jnp.where(high == piece, columns[piece * slab : (piece + 1) * slab], total)
            picked.append(total * LOG2E)
        return picked

    @pl.loop(0, tokens // 8)
    def _(block):
        rows = main_idx[pl.ds(pl.multiple_of(block * 8, 8), 8), :]
        for start in range(0, 8, AT_ONCE):
            lines = [rows[start + line : start + line + 1] for line in range(AT_ONCE)]
            for line, values in enumerate(lookup(lines)):
                bias[pl.ds(block * 8 + start + line, slab, stride=step), :] = values

    @pl.loop(0, rest // 8)
    def _(block):
        rows = rest_idx[pl.ds(pl.multiple_of(block * 8, 8), 8), :]
        for start in range(0, 8, AT_ONCE // 2):
            lines = []
            for line in range(start, start + AT_ONCE // 2):
                lines += [rows[line : line + 1, :LANES], rows[line : line + 1, LANES:]]
            for line, values in enumerate(lookup(lines)):
                base = tokens + rest * (line % 2)
                bias[pl.ds(base + block * 8 + start + line // 2, slab, stride=step), :] = values


def attend_window(heads, normed, query, key, row, bias, step, base, w_vt, turned):
    tokens, width = normed.shape
    dim = width // heads
    per = LANES // dim
    rest = tokens - LANES
    scale = dim ** (-0.5) * LOG2E
    value_t = lax.dot_general(w_vt[...], normed, NT, preferred_element_type=jnp.float32)
    value_t = value_t.astype(jnp.bfloat16)
    row = row.astype(jnp.float32)
    diagonal = lax.broadcasted_iota(jnp.int32, (tokens, tokens), 0) == lax.broadcasted_iota(
        jnp.int32, (tokens, tokens), 1
    )
    col = jnp.sum(jnp.where(diagonal, row, 0.0), axis=1, keepdims=True)
    barred = jnp.where(col == row[:, :LANES], 0.0, -jnp.inf)
    owner = lax.broadcasted_iota(jnp.int32, (LANES, LANES), 1) // dim
    zero = jnp.zeros((), jnp.bfloat16)
    for group in range(width // LANES):
        span = slice(group * LANES, (group + 1) * LANES)
        asked = query[:LANES, span]
        stacked = jnp.concatenate([jnp.where(owner == h, asked, zero) for h in range(per)], axis=0)
        raw = lax.dot_general(key[:, span], stacked, NT, preferred_element_type=jnp.float32)
        for h in range(per):
            head = group * per + h
            scores = raw[:, h * LANES : (h + 1) * LANES] * scale
            scores = scores + bias[base + head * step : base + head * step + tokens, :] + barred
            grown = jnp.exp2(scores - jnp.max(scores, axis=0, keepdims=True))
            total = jnp.sum(grown, axis=0, keepdims=True)
            mixed = jnp.dot(
                value_t[head * dim : (head + 1) * dim],
                grown.astype(jnp.bfloat16),
                preferred_element_type=jnp.float32,
            )
            turned[head * dim : (head + 1) * dim, :] = mixed / total
    owner = lax.broadcasted_iota(jnp.int32, (rest, width), 1) // dim
    asked = query[LANES:]
    stacked = jnp.concatenate([jnp.where(owner == h, asked, zero) for h in range(heads)], axis=0)
    scores = lax.dot_general(stacked, key, NT, preferred_element_type=jnp.float32) * scale
    starts = [base + h * step + tokens for h in range(heads)]
    left = jnp.concatenate([bias[start : start + rest, :] for start in starts], axis=0)
    right = jnp.concatenate([bias[start + rest : start + 2 * rest, :] for start in starts], axis=0)
    scores = scores + jnp.concatenate([left, right[:, : tokens - LANES]], axis=1)
    barred = jnp.where(col[LANES:] == row, 0.0, -jnp.inf)
    scores = scores + jnp.concatenate([barred] * heads, axis=0)
    grown = jnp.exp2(scores - jnp.max(scores, axis=1, keepdims=True))
    total = jnp.sum(grown, axis=1, keepdims=True)
    mixed = lax.dot_general(
        grown.astype(jnp.bfloat16), value_t, NT, preferred_element_type=jnp.float32
    )
    mixed = mixed / total
    last = jnp.zeros((rest, width), jnp.float32)
    for h in range(heads):
        last = jnp.where(owner == h, mixed[h * rest : (h + 1) * rest], last)
    return jnp.concatenate([turned[...].T, last], axis=0).astype(jnp.bfloat16)


def window_order(lat_wins, lon_wins):
    last_lat, last_lon = lat_wins - 1, lon_wins - 1
    order = [(t, last_lon) for t in range(lat_wins)]
    order += [(last_lat, b) for b in range(last_lon)]
    return order + [(t, b) for b in range(last_lon) for t in range(last_lat)]


def layer_kernel(
    heads, slab, step, regions, main_idx, rest_idx, fields, earth_far, qkv_far, proj_far, fc1_far,
    fc2_far, out, earth, w_qkv, w_proj, w_fc1, w_fc2, w_vt, table, bias, own, cols, rows, corner,
    wins, turned, cols_out, cols_back, tip_out, tip_back, rows_out, rows_back,
    load_sems, there_sems, here_sems, send_sems, take_sems,
):
    levels, lat_rows, lon_cols, width = own.shape
    lat_wins, lon_wins = lat_rows // WLAT, lon_cols // WLON
    last_lat, last_lon = lat_wins - 1, lon_wins - 1
    spare = corner.shape[2]
    tokens = wins.shape[1]
    dim = width // heads
    order = window_order(lat_wins, lon_wins)
    slot_of = {window: slot for slot, window in enumerate(order)}

    me_lat, me_lon = lax.axis_index("lat"), lax.axis_index("lon")
    lats, lons = lax.axis_size("lat"), lax.axis_size("lon")

    def device(lat, lon):
        return {
            "lat": lax.rem(me_lat + lat + lats, lats), "lon": lax.rem(me_lon + lon + lons, lons)
        }

    barrier = pltpu.get_barrier_semaphore()
    around = [(0, -1), (0, 1), (-1, 0), (1, 0), (-1, -1), (1, 1)]
    for where in around:
        pl.semaphore_signal(barrier, inc=1, device_id=device(*where), device_id_type=MESH)

    far = (earth_far, fields, qkv_far, proj_far, fc1_far, fc2_far)
    near = (earth, own, w_qkv, w_proj, w_fc1, w_fc2)
    loads = [
        pltpu.make_async_copy(source, target, load_sems.at[i])
        for i, (source, target) in enumerate(zip(far, near))
    ]
    for load in loads:
        load.start()

    def remote(source, target, sems, place, where):
        return pltpu.make_async_remote_copy(
            src_ref=source, dst_ref=target, send_sem=sems[0].at[place], recv_sem=sems[1].at[place],
            device_id=device(*where), device_id_type=MESH,
        )

    pl.semaphore_wait(barrier, len(around))
    ahead = []
    for t in range(lat_wins):
        low, high = t * WLAT + HALF_LAT, min((t + 1) * WLAT + HALF_LAT, lat_rows)
        ahead.append(
            remote(
                fields.at[:, low:high, :spare, :], cols.at[:, low:high], (there_sems, here_sems),
                t, (0, -1),
            )
        )
    tops = fields.at[:, :HALF_LAT]
    ahead.append(remote(tops, rows, (there_sems, here_sems), lat_wins, (-1, 0)))
    edge = fields.at[:, :HALF_LAT, :spare, :]
    ahead.append(remote(edge, corner, (there_sems, here_sems), lat_wins + 1, (-1, -1)))
    for copy in ahead[:last_lat]:
        copy.start()
    ahead[-1].start()
    ahead[last_lat].start()
    ahead[lat_wins].start()

    loads[0].wait()
    build_table(earth, table, slab)
    loads[2].wait()
    turn = w_qkv[:, 2 * width :].astype(jnp.float32).T
    w_vt[...] = turn.astype(jnp.bfloat16)

    fill_bias(main_idx, rest_idx, table, bias, slab, step)

    loads[1].wait()

    def gather(t):
        for level in range(levels):
            source = (level + WZ // 2) % levels
            for a in range(t * WLAT, (t + 1) * WLAT):
                away = a - (lat_rows - HALF_LAT)
                kept = own[source, a + HALF_LAT] if away < 0 else rows[source, away]
                halo = cols[source, a + HALF_LAT] if away < 0 else corner[source, away]
                line = [kept.astype(jnp.float32)[HALF_LON:], halo.astype(jnp.float32)[:HALF_LON]]
                line = jnp.concatenate(line, axis=0)
                place = (level * WLAT + a % WLAT) * WLON
                for b in range(lon_wins):
                    wins[slot_of[t, b], place : place + WLON, :] = line[b * WLON : (b + 1) * WLON]

    def send_back(result, t, b, base):
        copies = []
        count = levels * WLAT

        def lines(chosen, start, stop):
            parts = [result[base + k * WLON + start : base + k * WLON + stop] for k in chosen]
            return jnp.concatenate(parts, axis=0).astype(jnp.bfloat16)

        upper = [k for k in range(count) if k % WLAT < HALF_LAT]
        lower = [k for k in range(count) if k % WLAT >= HALF_LAT]
        sems = (send_sems, take_sems)
        if b == last_lon:
            if t < last_lat:
                cols_out[t] = lines(range(count), HALF_LON, WLON)
                copies.append(remote(cols_out.at[t], cols_back.at[t], sems, t, (0, 1)))
            else:
                tip_out[0] = lines(upper, HALF_LON, WLON)
                tip_out[1] = lines(lower, HALF_LON, WLON)
                copies.append(remote(tip_out.at[0], tip_back.at[0], sems, last_lat, (0, 1)))
                copies.append(remote(tip_out.at[1], tip_back.at[1], sems, lat_wins, (1, 1)))
        if t == last_lat:
            rows_out[b] = lines(lower, 0, WLON)
            copies.append(
                remote(rows_out.at[b], rows_back.at[b], sems, lat_wins + 1 + b, (1, 0))
            )
        for copy in copies:
            copy.start()
        return copies

    ready = set()
    returns = []
    for first in range(0, len(order), 2):
        group = order[first : first + 2]
        for t, b in group:
            if t in ready:
                continue
            ready.add(t)
            ahead[t].wait_recv()
            if t == last_lat:
                ahead[lat_wins].wait_recv()
                ahead[lat_wins + 1].wait_recv()
            gather(t)
        taken = wins[first : first + len(group)].reshape(len(group) * tokens, width)
        normed = norm_rows(taken)
        packed = jnp.dot(normed, w_qkv[:, : 2 * width], preferred_element_type=jnp.float32)
        packed = packed.astype(jnp.bfloat16)
        contexts = []
        for place, (t, b) in enumerate(group):
            part = slice(place * tokens, (place + 1) * tokens)
            contexts.append(
                attend_window(
                    heads, normed[part], packed[part, :width], packed[part, width:],
                    regions[t * lon_wins + b], bias, step, t * heads * step, w_vt,
                    turned.at[first + place],
                )
            )
        if first == 0:
            for load in loads[3:]:
                load.wait()
        context = jnp.concatenate(contexts, axis=0)
        projected = jnp.dot(context, w_proj[...], preferred_element_type=jnp.float32)
        projected = projected.astype(jnp.bfloat16).astype(jnp.float32)
        residual = (taken + projected).astype(jnp.bfloat16).astype(jnp.float32)
        normed = norm_rows(residual)
        grown = jnp.dot(normed, w_fc1[...], preferred_element_type=jnp.float32)
        hidden = (0.5 * grown * (1.0 + lax.erf(grown * math.sqrt(0.5)))).astype(jnp.bfloat16)
        summed = residual + jnp.dot(hidden, w_fc2[...], preferred_element_type=jnp.float32)
        wins[first : first + len(group)] = summed.reshape(len(group), tokens, width)
        for place, (t, b) in enumerate(group):
            returns += send_back(summed, t, b, place * tokens)

    for copy in ahead:
        copy.wait_send()
    for copy in returns:
        copy.wait()

    for level in range(levels):
        for r in range(lat_rows):
            if r < HALF_LAT:
                at = level * HALF_LAT + r
                kept = [rows_back[b, at * WLON : (at + 1) * WLON] for b in range(lon_wins)]
                halo = tip_back[1, at * HALF_LON : (at + 1) * HALF_LON]
            else:
                t, a = divmod(r - HALF_LAT, WLAT)
                at = level * WLAT + a
                kept = [wins[slot_of[t, b], at * WLON : (at + 1) * WLON] for b in range(lon_wins)]
                if t < last_lat:
                    halo = cols_back[t, at * HALF_LON : (at + 1) * HALF_LON]
                else:
                    at = level * HALF_LAT + a
                    halo = tip_back[0, at * HALF_LON : (at + 1) * HALF_LON]
            kept[-1] = kept[-1][:HALF_LON]
            line = jnp.concatenate([halo, *kept], axis=0) if r < HALF_LAT else jnp.concatenate(
                [halo.astype(jnp.float32), *kept], axis=0
            )
            out[(level + WZ // 2) % levels, r] = line.astype(jnp.bfloat16)


def local(fields, region_ids, bias_index, earth_bias, w_qkv, w_proj, w_fc1, w_fc2):
    levels, lat_rows, lon_cols, width = fields.shape
    lat_wins, lon_wins = lat_rows // WLAT, lon_cols // WLON
    tokens = levels * WLAT * WLON
    bands, positions, heads = earth_bias.shape
    rest = tokens - LANES
    spare = -(-HALF_LON // 8) * 8
    slab = -(-bands * heads // 8) * 8
    step = tokens + 2 * rest + 8
    pieces = -(-positions // LO)
    regions = region_ids.reshape(levels, lat_wins, WLAT, lon_wins, WLON)
    regions = regions.transpose(1, 3, 0, 2, 4).reshape(lat_wins * lon_wins, 1, tokens)
    main_idx = bias_index[:LANES].T
    rest_idx = jnp.pad(bias_index[LANES:], ((0, 0), (0, 2 * LANES - tokens)))
    count = lat_wins * lon_wins
    lines = levels * WLAT
    bf16, f32 = jnp.bfloat16, jnp.float32
    weights = (w_qkv, w_proj, w_fc1, w_fc2)
    near = pl.BlockSpec(memory_space=pltpu.VMEM)
    far = pl.BlockSpec(memory_space=pltpu.HBM)
    dma = pltpu.SemaphoreType.DMA
    scratch = [
        pltpu.VMEM(earth_bias.shape, bf16),
        *[pltpu.VMEM(weight.shape, bf16) for weight in weights],
        pltpu.VMEM((width, width), bf16),
        pltpu.VMEM((pieces * slab, LO), bf16),
        pltpu.VMEM((slab * step, LANES), f32),
        pltpu.VMEM(fields.shape, bf16),
        pltpu.VMEM((levels, lat_rows, spare, width), bf16),
        pltpu.VMEM((levels, HALF_LAT, lon_cols, width), bf16),
        pltpu.VMEM((levels, HALF_LAT, spare, width), bf16),
        pltpu.VMEM((count, tokens, width), f32),
        pltpu.VMEM((count, width, LANES), f32),
        pltpu.VMEM((max(lat_wins - 1, 1), lines * HALF_LON, width), bf16),
        pltpu.VMEM((max(lat_wins - 1, 1), lines * HALF_LON, width), bf16),
        pltpu.VMEM((2, lines // 2 * HALF_LON, width), bf16),
        pltpu.VMEM((2, lines // 2 * HALF_LON, width), bf16),
        pltpu.VMEM((lon_wins, lines // 2 * WLON, width), bf16),
        pltpu.VMEM((lon_wins, lines // 2 * WLON, width), bf16),
        dma((6,)),
        dma((lat_wins + 2,)),
        dma((lat_wins + 2,)),
        dma((lat_wins + 1 + lon_wins,)),
        dma((lat_wins + 1 + lon_wins,)),
    ]
    return pl.pallas_call(
        functools.partial(layer_kernel, heads, slab, step),
        out_shape=jax.ShapeDtypeStruct(fields.shape, bf16),
        in_specs=[near] * 3 + [far] * 6,
        out_specs=near,
        scratch_shapes=scratch,
        compiler_params=pltpu.CompilerParams(
            vmem_limit_bytes=GRANT, collective_id=0, has_side_effects=True
        ),
        cost_estimate=pl.CostEstimate(
            flops=2 * count * tokens * sum(weight.size for weight in weights),
            bytes_accessed=fields.size * 4 + earth_bias.size * 20,
            transcendentals=count * heads * tokens * tokens,
        ),
        name="layer",
    )(regions, main_idx, rest_idx, fields, earth_bias, *weights)


def solution(mesh):
    return jax.shard_map(
        local,
        mesh=mesh,
        in_specs=(
            P("ens", "lat", "lon", None),
            P(None, "lat", "lon"),
            P(),
            P("lat", None, None),
            P(),
            P(),
            P(),
            P(),
        ),
        out_specs=P("ens", "lat", "lon", None),
        check_vma=False,
    )
```

```python
import functools
import math

import jax
import jax.numpy as jnp
from jax import lax
from jax.experimental import pallas as pl
from jax.experimental.pallas import tpu as pltpu
from jax.sharding import PartitionSpec as P

WZ = 2
WLAT = 6
WLON = 12
HALF_LAT = WLAT // 2
HALF_LON = WLON // 2
EPS_NORM = 1e-05
LOG2E = math.log2(math.e)
LO = 256
LANES = 128
AT_ONCE = 4
EARLY = 4
MOST = (1, 2, 2, 2)
HEAD = 0
UNROLL = 7
GRANT = 64000000
NT = (((1,), (1,)), ((), ()))
MESH = pl.DeviceIdType.MESH


def norm_rows(wide):
    average = jnp.mean(wide, axis=-1, keepdims=True)
    centred = wide - average
    spread = jnp.mean(centred * centred, axis=-1, keepdims=True)
    return (centred * lax.rsqrt(spread + EPS_NORM)).astype(jnp.bfloat16)


def build_table(earth, table, slab):
    bands, heads, positions = earth.shape
    spare = jnp.zeros((slab - bands * heads, LO), jnp.float32)
    for piece in range(table.shape[0] // slab):
        start = piece * LO
        size = min(LO, positions - start)
        parts = [earth[band, :, start : start + size].astype(jnp.float32) for band in range(bands)]
        parts = [jnp.pad(part, ((0, 0), (0, LO - size))) for part in parts]
        rows = jnp.concatenate([*parts, spare][: bands + (slab > bands * heads)], axis=0)
        table[piece * slab : (piece + 1) * slab, :] = rows.astype(jnp.bfloat16)


def split_index(index, main_idx, rest_idx):
    tokens = index.shape[0]
    wide = jnp.pad(index[...], ((0, 0), (0, 2 * LANES - tokens)))
    main_idx[...] = wide[:LANES].T[:tokens]
    rest_idx[...] = wide[LANES:]


def fill_bias(main_idx, rest_idx, table, bias, slab, step, begin, end, unroll):
    tokens = main_idx.shape[0]
    rest = rest_idx.shape[0]
    pieces = table.shape[0] // slab
    low = lax.broadcasted_iota(jnp.int32, (LO, LANES), 0).astype(jnp.bfloat16)
    one, zero = jnp.ones((), jnp.bfloat16), jnp.zeros((), jnp.bfloat16)

    def lookup(lines):
        rows = [(line & (LO - 1)).astype(jnp.bfloat16) for line in lines]
        spots = jnp.concatenate([jnp.where(low == row, one, zero) for row in rows], axis=1)
        found = jnp.dot(table[...], spots, preferred_element_type=jnp.float32)
        high = [line // LO for line in lines]
        total = [found[:slab, i * LANES : (i + 1) * LANES] for i in range(len(lines))]
        for piece in range(1, pieces):
            for i in range(len(lines)):
                here = found[piece * slab : (piece + 1) * slab, i * LANES : (i + 1) * LANES]
                total[i] = jnp.where(high[i] == piece, here, total[i])
        return [values * LOG2E for values in total]

    @pl.loop(begin, end, unroll=math.gcd(end - begin, unroll))
    def _(block):
        rows = main_idx[pl.ds(pl.multiple_of(block * 8, 8), 8), :]
        for start in range(0, 8, AT_ONCE):
            lines = [rows[start + line : start + line + 1] for line in range(AT_ONCE)]
            for line, values in enumerate(lookup(lines)):
                bias[pl.ds(block * 8 + start + line, slab, stride=step), :] = values

    if end < tokens // 8:
        return

    @pl.loop(0, rest // 8)
    def _(block):
        rows = rest_idx[pl.ds(pl.multiple_of(block * 8, 8), 8), :]
        for start in range(0, 8, AT_ONCE // 2):
            lines = []
            for line in range(start, start + AT_ONCE // 2):
                lines += [rows[line : line + 1, :LANES], rows[line : line + 1, LANES:]]
            for line, values in enumerate(lookup(lines)):
                base = tokens + rest * (line % 2)
                bias[pl.ds(base + block * 8 + start + line // 2, slab, stride=step), :] = values


def attend_window(heads, normed, query, key, row, bias, step, base, w_vt, turned):
    tokens, width = normed.shape
    dim = width // heads
    per = LANES // dim
    rest = tokens - LANES
    scale = dim ** (-0.5) * LOG2E
    value_t = lax.dot_general(w_vt[...], normed, NT, preferred_element_type=jnp.float32)
    value_t = value_t.astype(jnp.bfloat16)
    row = row.astype(jnp.float32)
    diagonal = lax.broadcasted_iota(jnp.int32, (tokens, tokens), 0) == lax.broadcasted_iota(
        jnp.int32, (tokens, tokens), 1
    )
    col = jnp.sum(jnp.where(diagonal, row, 0.0), axis=1, keepdims=True)
    barred = jnp.where(col == row[:, :LANES], 0.0, -jnp.inf)
    owner = lax.broadcasted_iota(jnp.int32, (LANES, LANES), 1) // dim
    zero = jnp.zeros((), jnp.bfloat16)
    for group in range(width // LANES):
        span = slice(group * LANES, (group + 1) * LANES)
        asked = query[:LANES, span]
        stacked = jnp.concatenate([jnp.where(owner == h, asked, zero) for h in range(per)], axis=0)
        raw = lax.dot_general(key[:, span], stacked, NT, preferred_element_type=jnp.float32)
        for h in range(per):
            head = group * per + h
            scores = raw[:, h * LANES : (h + 1) * LANES] * scale
            scores = scores + bias[base + head * step : base + head * step + tokens, :] + barred
            grown = jnp.exp2(scores - jnp.max(scores, axis=0, keepdims=True))
            total = jnp.sum(grown, axis=0, keepdims=True)
            mixed = jnp.dot(
                value_t[head * dim : (head + 1) * dim],
                grown.astype(jnp.bfloat16),
                preferred_element_type=jnp.float32,
            )
            turned[head * dim : (head + 1) * dim, :] = mixed / total
    owner = lax.broadcasted_iota(jnp.int32, (rest, width), 1) // dim
    asked = query[LANES:]
    stacked = jnp.concatenate([jnp.where(owner == h, asked, zero) for h in range(heads)], axis=0)
    scores = lax.dot_general(stacked, key, NT, preferred_element_type=jnp.float32) * scale
    starts = [base + h * step + tokens for h in range(heads)]
    left = jnp.concatenate([bias[start : start + rest, :] for start in starts], axis=0)
    right = jnp.concatenate([bias[start + rest : start + 2 * rest, :] for start in starts], axis=0)
    scores = scores + jnp.concatenate([left, right[:, : tokens - LANES]], axis=1)
    barred = jnp.where(col[LANES:] == row, 0.0, -jnp.inf)
    scores = scores + jnp.concatenate([barred] * heads, axis=0)
    grown = jnp.exp2(scores - jnp.max(scores, axis=1, keepdims=True))
    total = jnp.sum(grown, axis=1, keepdims=True)
    mixed = lax.dot_general(
        grown.astype(jnp.bfloat16), value_t, NT, preferred_element_type=jnp.float32
    )
    mixed = mixed / total
    last = jnp.zeros((rest, width), jnp.float32)
    for h in range(heads):
        last = jnp.where(owner == h, mixed[h * rest : (h + 1) * rest], last)
    return jnp.concatenate([turned[...].T, last], axis=0).astype(jnp.bfloat16)


def window_groups(lat_wins, lon_wins):
    last_lat, last_lon = lat_wins - 1, lon_wins - 1
    inner = [(t, b) for b in range(last_lon) for t in range(last_lat)]
    kinds = [
        inner[:HEAD],
        [(t, last_lon) for t in range(lat_wins)],
        [(last_lat, b) for b in range(last_lon)],
        inner[HEAD:],
    ]
    return [
        kind[first : first + most]
        for kind, most in zip(kinds, MOST)
        for first in range(0, len(kind), most)
    ]


def layer_kernel(
    heads, slab, step, index_far, regions_far, fields, earth_far, qkv_far, proj_far, fc1_far,
    fc2_far, out, index, regions, earth, w_qkv, w_proj, w_fc1, w_fc2, w_vt, main_idx, rest_idx,
    table, bias, own, cols, rows, corner,
    wins, turned, cols_out, cols_back, tip_out, tip_back, rows_out, rows_back,
    load_sems, there_sems, here_sems, send_sems, take_sems,
):
    levels, lat_rows, lon_cols, width = own.shape
    lat_wins, lon_wins = lat_rows // WLAT, lon_cols // WLON
    last_lat, last_lon = lat_wins - 1, lon_wins - 1
    spare = corner.shape[2]
    tokens = wins.shape[1]
    dim = width // heads
    groups = window_groups(lat_wins, lon_wins)
    order = sum(groups, [])
    slot_of = {window: slot for slot, window in enumerate(order)}

    me_lat, me_lon = lax.axis_index("lat"), lax.axis_index("lon")
    lats, lons = lax.axis_size("lat"), lax.axis_size("lon")

    def device(lat, lon):
        return {
            "lat": lax.rem(me_lat + lat + lats, lats), "lon": lax.rem(me_lon + lon + lons, lons)
        }

    barrier = pltpu.get_barrier_semaphore()
    around = [(0, -1), (0, 1), (-1, 0), (1, 0), (-1, -1), (1, 1)]
    for where in around:
        pl.semaphore_signal(barrier, inc=1, device_id=device(*where), device_id_type=MESH)

    far = (earth_far, index_far, regions_far, fields, qkv_far, proj_far, fc1_far, fc2_far)
    near = (earth, index, regions, own, w_qkv, w_proj, w_fc1, w_fc2)
    loads = [
        pltpu.make_async_copy(source, target, load_sems.at[i])
        for i, (source, target) in enumerate(zip(far, near))
    ]
    for load in loads:
        load.start()

    def remote(source, target, sems, place, where):
        return pltpu.make_async_remote_copy(
            src_ref=source, dst_ref=target, send_sem=sems[0].at[place], recv_sem=sems[1].at[place],
            device_id=device(*where), device_id_type=MESH,
        )

    ahead = []
    for t in range(lat_wins):
        low, high = t * WLAT + HALF_LAT, min((t + 1) * WLAT + HALF_LAT, lat_rows)
        ahead.append(
            remote(
                fields.at[:, low:high, :spare, :], cols.at[:, low:high], (there_sems, here_sems),
                t, (0, -1),
            )
        )
    tops = fields.at[:, :HALF_LAT]
    ahead.append(remote(tops, rows, (there_sems, here_sems), lat_wins, (-1, 0)))
    edge = fields.at[:, :HALF_LAT, :spare, :]
    ahead.append(remote(edge, corner, (there_sems, here_sems), lat_wins + 1, (-1, -1)))

    loads[0].wait()
    build_table(earth, table, slab)
    loads[1].wait()
    split_index(index, main_idx, rest_idx)
    loads[4].wait()
    turn = w_qkv[:, 2 * width :].astype(jnp.float32).T
    w_vt[...] = turn.astype(jnp.bfloat16)

    blocks = tokens // 8
    fill_bias(main_idx, rest_idx, table, bias, slab, step, 0, EARLY, EARLY)
    pl.semaphore_wait(barrier, len(around))
    for copy in ahead[:last_lat]:
        copy.start()
    ahead[-1].start()
    ahead[last_lat].start()
    ahead[lat_wins].start()
    fill_bias(main_idx, rest_idx, table, bias, slab, step, EARLY, blocks, UNROLL)

    loads[2].wait()
    loads[3].wait()

    def gather(t, b):
        span = slice(b * WLON, (b + 1) * WLON)
        for level in range(levels):
            source = (level + WZ // 2) % levels
            for a in range(t * WLAT, (t + 1) * WLAT):
                away = a - (lat_rows - HALF_LAT)
                kept = own[source, a + HALF_LAT] if away < 0 else rows[source, away]
                line = kept.astype(jnp.float32)[HALF_LON:]
                if b == last_lon:
                    halo = cols[source, a + HALF_LAT] if away < 0 else corner[source, away]
                    line = jnp.concatenate([line, halo.astype(jnp.float32)[:HALF_LON]], axis=0)
                place = (level * WLAT + a % WLAT) * WLON
                wins[slot_of[t, b], place : place + WLON, :] = line[span]

    def region_row(t, b):
        span = slice(b * WLON, (b + 1) * WLON)
        parts = [
            regions[t * WLAT + a, level : level + 1, span]
            for level in range(levels)
            for a in range(WLAT)
        ]
        return jnp.concatenate(parts, axis=1)

    def send_back(result, t, b, base):
        copies = []
        count = levels * WLAT

        def lines(chosen, start, stop):
            parts = [result[base + k * WLON + start : base + k * WLON + stop] for k in chosen]
            return jnp.concatenate(parts, axis=0).astype(jnp.bfloat16)

        upper = [k for k in range(count) if k % WLAT < HALF_LAT]
        lower = [k for k in range(count) if k % WLAT >= HALF_LAT]
        sems = (send_sems, take_sems)
        if b == last_lon:
            if t < last_lat:
                cols_out[t] = lines(range(count), HALF_LON, WLON)
                copies.append(remote(cols_out.at[t], cols_back.at[t], sems, t, (0, 1)))
            else:
                tip_out[0] = lines(upper, HALF_LON, WLON)
                tip_out[1] = lines(lower, HALF_LON, WLON)
                copies.append(remote(tip_out.at[0], tip_back.at[0], sems, last_lat, (0, 1)))
                copies.append(remote(tip_out.at[1], tip_back.at[1], sems, lat_wins, (1, 1)))
        if t == last_lat:
            rows_out[b] = lines(lower, 0, WLON)
            copies.append(
                remote(rows_out.at[b], rows_back.at[b], sems, lat_wins + 1 + b, (1, 0))
            )
        for copy in copies:
            copy.start()
        return copies

    ready = set()
    returns = []
    for group in groups:
        first = slot_of[group[0]]
        for t, b in group:
            needed = {t} if b == last_lon else set()
            if t == last_lat:
                needed |= {lat_wins, lat_wins + 1} if b == last_lon else {lat_wins}
            for which in sorted(needed - ready):
                ahead[which].wait_recv()
            ready |= needed
            gather(t, b)
        taken = wins[first : first + len(group)].reshape(len(group) * tokens, width)
        normed = norm_rows(taken)
        packed = jnp.dot(normed, w_qkv[:, : 2 * width], preferred_element_type=jnp.float32)
        packed = packed.astype(jnp.bfloat16)
        contexts = []
        for place, (t, b) in enumerate(group):
            part = slice(place * tokens, (place + 1) * tokens)
            contexts.append(
                attend_window(
                    heads, normed[part], packed[part, :width], packed[part, width:],
                    region_row(t, b), bias, step, t * heads * step, w_vt,
                    turned.at[first + place],
                )
            )
        if group is groups[0]:
            for load in loads[5:]:
                load.wait()
        context = jnp.concatenate(contexts, axis=0)
        projected = jnp.dot(context, w_proj[...], preferred_element_type=jnp.float32)
        projected = projected.astype(jnp.bfloat16).astype(jnp.float32)
        residual = (taken + projected).astype(jnp.bfloat16).astype(jnp.float32)
        normed = norm_rows(residual)
        grown = jnp.dot(normed, w_fc1[...], preferred_element_type=jnp.float32)
        hidden = (0.5 * grown * (1.0 + lax.erf(grown * math.sqrt(0.5)))).astype(jnp.bfloat16)
        summed = residual + jnp.dot(hidden, w_fc2[...], preferred_element_type=jnp.float32)
        wins[first : first + len(group)] = summed.reshape(len(group), tokens, width)
        for place, (t, b) in enumerate(group):
            returns += send_back(summed, t, b, place * tokens)

    for copy in ahead:
        copy.wait_send()
    for copy in returns:
        copy.wait()

    for level in range(levels):
        for r in range(lat_rows):
            if r < HALF_LAT:
                at = level * HALF_LAT + r
                kept = [rows_back[b, at * WLON : (at + 1) * WLON] for b in range(lon_wins)]
                halo = tip_back[1, at * HALF_LON : (at + 1) * HALF_LON]
            else:
                t, a = divmod(r - HALF_LAT, WLAT)
                at = level * WLAT + a
                kept = [wins[slot_of[t, b], at * WLON : (at + 1) * WLON] for b in range(lon_wins)]
                if t < last_lat:
                    halo = cols_back[t, at * HALF_LON : (at + 1) * HALF_LON]
                else:
                    at = level * HALF_LAT + a
                    halo = tip_back[0, at * HALF_LON : (at + 1) * HALF_LON]
            kept[-1] = kept[-1][:HALF_LON]
            line = jnp.concatenate([halo, *kept], axis=0) if r < HALF_LAT else jnp.concatenate(
                [halo.astype(jnp.float32), *kept], axis=0
            )
            out[(level + WZ // 2) % levels, r] = line.astype(jnp.bfloat16)


def local(fields, region_ids, bias_index, earth_bias, w_qkv, w_proj, w_fc1, w_fc2):
    levels, lat_rows, lon_cols, width = fields.shape
    lat_wins, lon_wins = lat_rows // WLAT, lon_cols // WLON
    tokens = levels * WLAT * WLON
    bands, positions, heads = earth_bias.shape
    rest = tokens - LANES
    spare = -(-HALF_LON // 8) * 8
    slab = -(-bands * heads // 8) * 8
    step = tokens + 2 * rest + 8
    pieces = -(-positions // LO)
    count = lat_wins * lon_wins
    lines = levels * WLAT
    bf16, f32 = jnp.bfloat16, jnp.float32
    weights = (w_qkv, w_proj, w_fc1, w_fc2)
    near = pl.BlockSpec(memory_space=pltpu.VMEM)
    far = pl.BlockSpec(memory_space=pltpu.HBM)
    dma = pltpu.SemaphoreType.DMA
    scratch = [
        pltpu.VMEM(bias_index.shape, jnp.int32),
        pltpu.VMEM((lat_rows, levels, lon_cols), jnp.int32),
        pltpu.VMEM((bands, heads, positions), bf16),
        *[pltpu.VMEM(weight.shape, bf16) for weight in weights],
        pltpu.VMEM((width, width), bf16),
        pltpu.VMEM((tokens, LANES), jnp.int32),
        pltpu.VMEM((rest, 2 * LANES), jnp.int32),
        pltpu.VMEM((pieces * slab, LO), bf16),
        pltpu.VMEM((slab * step, LANES), f32),
        pltpu.VMEM(fields.shape, bf16),
        pltpu.VMEM((levels, lat_rows, spare, width), bf16),
        pltpu.VMEM((levels, HALF_LAT, lon_cols, width), bf16),
        pltpu.VMEM((levels, HALF_LAT, spare, width), bf16),
        pltpu.VMEM((count, tokens, width), f32),
        pltpu.VMEM((count, width, LANES), f32),
        pltpu.VMEM((max(lat_wins - 1, 1), lines * HALF_LON, width), bf16),
        pltpu.VMEM((max(lat_wins - 1, 1), lines * HALF_LON, width), bf16),
        pltpu.VMEM((2, lines // 2 * HALF_LON, width), bf16),
        pltpu.VMEM((2, lines // 2 * HALF_LON, width), bf16),
        pltpu.VMEM((lon_wins, lines // 2 * WLON, width), bf16),
        pltpu.VMEM((lon_wins, lines // 2 * WLON, width), bf16),
        dma((8,)),
        dma((lat_wins + 2,)),
        dma((lat_wins + 2,)),
        dma((lat_wins + 1 + lon_wins,)),
        dma((lat_wins + 1 + lon_wins,)),
    ]
    return pl.pallas_call(
        functools.partial(layer_kernel, heads, slab, step),
        out_shape=pltpu.VMEM(fields.shape, bf16),
        in_specs=[far] * 8,
        out_specs=near,
        scratch_shapes=scratch,
        compiler_params=pltpu.CompilerParams(
            vmem_limit_bytes=GRANT, collective_id=0, has_side_effects=True
        ),
        cost_estimate=pl.CostEstimate(
            flops=2 * count * tokens * sum(weight.size for weight in weights),
            bytes_accessed=fields.size * 4 + earth_bias.size * 20,
            transcendentals=count * heads * tokens * tokens,
        ),
        name="layer",
    )(
        bias_index, region_ids.transpose(1, 0, 2), fields, earth_bias.transpose(0, 2, 1), *weights
    )


def solution(mesh):
    return jax.shard_map(
        local,
        mesh=mesh,
        in_specs=(
            P("ens", "lat", "lon", None),
            P(None, "lat", "lon"),
            P(),
            P("lat", None, None),
            P(),
            P(),
            P(),
            P(),
        ),
        out_specs=P("ens", "lat", "lon", None),
        check_vma=False,
    )
```

```python
import functools
import math

import jax
import jax.numpy as jnp
from jax import lax
from jax.experimental import pallas as pl
from jax.experimental.pallas import tpu as pltpu
from jax.sharding import PartitionSpec as P

WZ = 2
WLAT = 6
WLON = 12
HALF_LAT = WLAT // 2
HALF_LON = WLON // 2
EPS_NORM = 1e-05
LOG2E = math.log2(math.e)
LO = 256
LANES = 128
AT_ONCE = 4
EARLY = 2
MOST = (2, 2, 2, 2)
HEAD = 0
UNROLL = 8
CHUNK = 256
GRANT = 64000000
NT = (((1,), (1,)), ((), ()))
MESH = pl.DeviceIdType.MESH


def norm_rows(wide):
    average = jnp.mean(wide, axis=-1, keepdims=True)
    centred = wide - average
    spread = jnp.mean(centred * centred, axis=-1, keepdims=True)
    return (centred * lax.rsqrt(spread + EPS_NORM)).astype(jnp.bfloat16)


def table_rows(count, pieces):
    whole = count // 8 * 8
    left = count - whole
    fold = 8 // left if left else 1
    tiles = -(-pieces // fold) if left else 0
    return whole, left, fold, tiles


def build_table(earth, table):
    bands, heads, positions = earth.shape
    pieces = -(-positions // LO)
    whole, left, fold, tiles = table_rows(bands * heads, pieces)
    ends = []
    for piece in range(pieces):
        start = piece * LO
        size = min(LO, positions - start)
        parts = [earth[band, :, start : start + size].astype(jnp.float32) for band in range(bands)]
        parts = [jnp.pad(part, ((0, 0), (0, LO - size))) for part in parts]
        rows = jnp.concatenate(parts, axis=0)
        table[piece * whole : (piece + 1) * whole, :] = rows[:whole].astype(jnp.bfloat16)
        ends.append(rows[whole:])
    if left:
        base = pieces * whole
        for tile in range(tiles):
            rows = ends[tile * fold : (tile + 1) * fold]
            spare = 8 - left * len(rows)
            if spare:
                rows = [*rows, jnp.zeros((spare, LO), jnp.float32)]
            rows = jnp.concatenate(rows, axis=0).astype(jnp.bfloat16)
            table[base + tile * 8 : base + (tile + 1) * 8, :] = rows


def split_index(index, main_idx, left_idx, right_idx):
    tokens = index.shape[0]
    rest = tokens - LANES
    wide = jnp.pad(index[...], ((0, 0), (0, 2 * LANES - tokens)))
    main_idx[...] = wide[:LANES].T[:tokens]
    left_idx[...] = wide[LANES:, :LANES]
    beside = LANES // rest
    corner = wide[LANES:, LANES:]
    for line in range(rest // beside):
        parts = [corner[line * beside + i : line * beside + i + 1, :rest] for i in range(beside)]
        right_idx[line : line + 1, :] = jnp.concatenate(parts, axis=1)


def fill_bias(main_idx, left_idx, right_idx, table, bias, count, pieces, step, begin, end, unroll):
    tokens = main_idx.shape[0]
    rest = left_idx.shape[0]
    whole, left, fold, tiles = table_rows(count, pieces)
    low = lax.broadcasted_iota(jnp.int32, (LO, LANES), 0).astype(jnp.bfloat16)
    one, zero = jnp.ones((), jnp.bfloat16), jnp.zeros((), jnp.bfloat16)

    def lookup(lines):
        rows = [(line & (LO - 1)).astype(jnp.bfloat16) for line in lines]
        spots = jnp.concatenate([jnp.where(low == row, one, zero) for row in rows], axis=1)
        found = jnp.dot(table[...], spots, preferred_element_type=jnp.float32)
        high = [line // LO for line in lines]
        spans = [slice(i * LANES, (i + 1) * LANES) for i in range(len(lines))]
        total = [found[:whole, span] for span in spans]
        for piece in range(1, pieces):
            for i, span in enumerate(spans):
                here = found[piece * whole : (piece + 1) * whole, span]
                total[i] = jnp.where(high[i] == piece, here, total[i])
        if left:
            base = pieces * whole
            ends = [found[base : base + 8, span] for span in spans]
            for tile in range(1, tiles):
                for i, span in enumerate(spans):
                    here = found[base + tile * 8 : base + (tile + 1) * 8, span]
                    ends[i] = jnp.where(high[i] // fold == tile, here, ends[i])
            for i, end in enumerate(ends):
                picked = end[:left]
                for part in range(1, fold):
                    here = end[part * left : (part + 1) * left]
                    picked = jnp.where(high[i] % fold == part, here, picked)
                total[i] = (total[i], picked)
        else:
            total = [(values, None) for values in total]
        return total

    def keep(place, values):
        bias[pl.ds(place, whole, stride=step), :] = values[0] * LOG2E
        if left:
            bias[pl.ds(place + whole * step, left, stride=step), :] = values[1] * LOG2E

    @pl.loop(begin, end, unroll=math.gcd(end - begin, unroll))
    def _(block):
        rows = main_idx[pl.ds(pl.multiple_of(block * 8, 8), 8), :]
        for start in range(0, 8, AT_ONCE):
            lines = [rows[start + line : start + line + 1] for line in range(AT_ONCE)]
            for line, values in enumerate(lookup(lines)):
                keep(block * 8 + start + line, values)

    if end < tokens // 8:
        return

    for start in range(0, rest, AT_ONCE):
        lines = [left_idx[line : line + 1, :] for line in range(start, min(start + AT_ONCE, rest))]
        for line, values in enumerate(lookup(lines)):
            keep(tokens + start + line, values)
    beside = LANES // rest
    lines = [right_idx[line : line + 1, :] for line in range(rest // beside)]
    for line, values in enumerate(lookup(lines)):
        for i in range(beside):
            turned = [
                part if part is None or i == 0 else pltpu.roll(part, LANES - i * rest, axis=1)
                for part in values
            ]
            keep(tokens + rest + line * beside + i, turned)


def attend_window(heads, normed, query, key, row, bias, step, base, w_vt, turned):
    tokens, width = normed.shape
    dim = width // heads
    per = LANES // dim
    rest = tokens - LANES
    scale = dim ** (-0.5) * LOG2E
    value_t = lax.dot_general(w_vt[...], normed, NT, preferred_element_type=jnp.float32)
    value_t = value_t.astype(jnp.bfloat16)
    row = row.astype(jnp.float32)
    diagonal = lax.broadcasted_iota(jnp.int32, (tokens, tokens), 0) == lax.broadcasted_iota(
        jnp.int32, (tokens, tokens), 1
    )
    col = jnp.sum(jnp.where(diagonal, row, 0.0), axis=1, keepdims=True)
    barred = jnp.where(col == row[:, :LANES], 0.0, -jnp.inf)
    owner = lax.broadcasted_iota(jnp.int32, (LANES, LANES), 1) // dim
    zero = jnp.zeros((), jnp.bfloat16)
    for group in range(width // LANES):
        span = slice(group * LANES, (group + 1) * LANES)
        asked = query[:LANES, span]
        stacked = jnp.concatenate([jnp.where(owner == h, asked, zero) for h in range(per)], axis=0)
        raw = lax.dot_general(key[:, span], stacked, NT, preferred_element_type=jnp.float32)
        for h in range(per):
            head = group * per + h
            scores = raw[:, h * LANES : (h + 1) * LANES] * scale
            scores = scores + bias[base + head * step : base + head * step + tokens, :] + barred
            grown = jnp.exp2(scores - jnp.max(scores, axis=0, keepdims=True))
            total = jnp.sum(grown, axis=0, keepdims=True)
            mixed = jnp.dot(
                value_t[head * dim : (head + 1) * dim],
                grown.astype(jnp.bfloat16),
                preferred_element_type=jnp.float32,
            )
            turned[head * dim : (head + 1) * dim, :] = mixed / total
        yield
    owner = lax.broadcasted_iota(jnp.int32, (rest, width), 1) // dim
    asked = query[LANES:]
    stacked = jnp.concatenate([jnp.where(owner == h, asked, zero) for h in range(heads)], axis=0)
    scores = lax.dot_general(stacked, key, NT, preferred_element_type=jnp.float32) * scale
    starts = [base + h * step + tokens for h in range(heads)]
    left = jnp.concatenate([bias[start : start + rest, :] for start in starts], axis=0)
    right = jnp.concatenate([bias[start + rest : start + 2 * rest, :] for start in starts], axis=0)
    scores = scores + jnp.concatenate([left, right[:, : tokens - LANES]], axis=1)
    barred = jnp.where(col[LANES:] == row, 0.0, -jnp.inf)
    scores = scores + jnp.concatenate([barred] * heads, axis=0)
    grown = jnp.exp2(scores - jnp.max(scores, axis=1, keepdims=True))
    total = jnp.sum(grown, axis=1, keepdims=True)
    mixed = lax.dot_general(
        grown.astype(jnp.bfloat16), value_t, NT, preferred_element_type=jnp.float32
    )
    mixed = mixed / total
    last = jnp.zeros((rest, width), jnp.float32)
    for h in range(heads):
        last = jnp.where(owner == h, mixed[h * rest : (h + 1) * rest], last)
    yield jnp.concatenate([turned[...].T, last], axis=0).astype(jnp.bfloat16)


def feed_forward(residual, normed, w_fc1, w_fc2):
    hidden = []
    for start in range(0, w_fc1.shape[1], CHUNK):
        grown = jnp.dot(
            normed, w_fc1[:, start : start + CHUNK], preferred_element_type=jnp.float32
        )
        halved = 0.5 * grown * (1.0 + lax.erf(grown * math.sqrt(0.5)))
        hidden.append(halved.astype(jnp.bfloat16))
        yield
    hidden = jnp.concatenate(hidden, axis=1)
    yield residual + jnp.dot(hidden, w_fc2[...], preferred_element_type=jnp.float32)


def weave(*works):
    steps = [count for work, count in works]
    done, values = [0] * len(works), [None] * len(works)
    for _ in range(sum(steps)):
        which = min(
            (i for i in range(len(works)) if done[i] < steps[i]),
            key=lambda i: (done[i] + 0.5) / steps[i],
        )
        values[which] = next(works[which][0])
        done[which] += 1
    return values


def window_groups(lat_wins, lon_wins):
    last_lat, last_lon = lat_wins - 1, lon_wins - 1
    inner = [(t, b) for b in range(last_lon) for t in range(last_lat)]
    kinds = [
        inner[:HEAD],
        [(t, last_lon) for t in range(lat_wins)],
        [(last_lat, b) for b in range(last_lon)],
        inner[HEAD:],
    ]
    return [
        kind[first : first + most]
        for kind, most in zip(kinds, MOST)
        for first in range(0, len(kind), most)
    ]


def layer_kernel(
    heads, step, index_far, regions_far, fields, earth_far, qkv_far, proj_far, fc1_far,
    fc2_far, out, index, regions, earth, w_qkv, w_proj, w_fc1, w_fc2, w_vt, main_idx, left_idx,
    right_idx, table, bias, own, cols, rows, corner,
    wins, turned, cols_out, cols_back, tip_out, tip_back, rows_out, rows_back,
    load_sems, there_sems, here_sems, send_sems, take_sems,
):
    levels, lat_rows, lon_cols, width = own.shape
    lat_wins, lon_wins = lat_rows // WLAT, lon_cols // WLON
    last_lat, last_lon = lat_wins - 1, lon_wins - 1
    spare = corner.shape[2]
    tokens = wins.shape[1]
    dim = width // heads
    groups = window_groups(lat_wins, lon_wins)
    order = sum(groups, [])
    slot_of = {window: slot for slot, window in enumerate(order)}

    me_lat, me_lon = lax.axis_index("lat"), lax.axis_index("lon")
    lats, lons = lax.axis_size("lat"), lax.axis_size("lon")

    def device(lat, lon):
        return {
            "lat": lax.rem(me_lat + lat + lats, lats), "lon": lax.rem(me_lon + lon + lons, lons)
        }

    barrier = pltpu.get_barrier_semaphore()
    around = [(0, -1), (0, 1), (-1, 0), (1, 0), (-1, -1), (1, 1)]
    for where in around:
        pl.semaphore_signal(barrier, inc=1, device_id=device(*where), device_id_type=MESH)

    far = (earth_far, index_far, regions_far, fields, qkv_far, proj_far, fc1_far, fc2_far)
    near = (earth, index, regions, own, w_qkv, w_proj, w_fc1, w_fc2)
    loads = [
        pltpu.make_async_copy(source, target, load_sems.at[i])
        for i, (source, target) in enumerate(zip(far, near))
    ]
    for load in loads:
        load.start()

    def remote(source, target, sems, place, where):
        return pltpu.make_async_remote_copy(
            src_ref=source, dst_ref=target, send_sem=sems[0].at[place], recv_sem=sems[1].at[place],
            device_id=device(*where), device_id_type=MESH,
        )

    ahead = []
    for t in range(lat_wins):
        low, high = t * WLAT + HALF_LAT, min((t + 1) * WLAT + HALF_LAT, lat_rows)
        ahead.append(
            remote(
                fields.at[:, low:high, :spare, :], cols.at[:, low:high], (there_sems, here_sems),
                t, (0, -1),
            )
        )
    tops = fields.at[:, :HALF_LAT]
    ahead.append(remote(tops, rows, (there_sems, here_sems), lat_wins, (-1, 0)))
    edge = fields.at[:, :HALF_LAT, :spare, :]
    ahead.append(remote(edge, corner, (there_sems, here_sems), lat_wins + 1, (-1, -1)))

    loads[0].wait()
    build_table(earth, table)
    loads[1].wait()
    split_index(index, main_idx, left_idx, right_idx)
    loads[4].wait()
    turn = w_qkv[:, 2 * width :].astype(jnp.float32).T
    w_vt[...] = turn.astype(jnp.bfloat16)

    blocks = tokens // 8
    look = functools.partial(
        fill_bias, main_idx, left_idx, right_idx, table, bias, earth.shape[0] * heads,
        -(-earth.shape[2] // LO), step,
    )
    look(0, EARLY, EARLY)
    pl.semaphore_wait(barrier, len(around))
    for copy in ahead[:last_lat]:
        copy.start()
    ahead[-1].start()
    ahead[last_lat].start()
    ahead[lat_wins].start()
    look(EARLY, blocks, UNROLL)

    loads[2].wait()
    loads[3].wait()

    def gather(t, b):
        span = slice(b * WLON, (b + 1) * WLON)
        for level in range(levels):
            source = (level + WZ // 2) % levels
            for a in range(t * WLAT, (t + 1) * WLAT):
                away = a - (lat_rows - HALF_LAT)
                kept = own[source, a + HALF_LAT] if away < 0 else rows[source, away]
                line = kept.astype(jnp.float32)[HALF_LON:]
                if b == last_lon:
                    halo = cols[source, a + HALF_LAT] if away < 0 else corner[source, away]
                    line = jnp.concatenate([line, halo.astype(jnp.float32)[:HALF_LON]], axis=0)
                place = (level * WLAT + a % WLAT) * WLON
                wins[slot_of[t, b], place : place + WLON, :] = line[span]

    def region_row(t, b):
        span = slice(b * WLON, (b + 1) * WLON)
        parts = [
            regions[t * WLAT + a, level : level + 1, span]
            for level in range(levels)
            for a in range(WLAT)
        ]
        return jnp.concatenate(parts, axis=1)

    def send_back(result, t, b, base):
        copies = []
        count = levels * WLAT

        def lines(chosen, start, stop):
            parts = [result[base + k * WLON + start : base + k * WLON + stop] for k in chosen]
            return jnp.concatenate(parts, axis=0).astype(jnp.bfloat16)

        upper = [k for k in range(count) if k % WLAT < HALF_LAT]
        lower = [k for k in range(count) if k % WLAT >= HALF_LAT]
        sems = (send_sems, take_sems)
        if b == last_lon:
            if t < last_lat:
                cols_out[t] = lines(range(count), HALF_LON, WLON)
                copies.append(remote(cols_out.at[t], cols_back.at[t], sems, t, (0, 1)))
            else:
                tip_out[0] = lines(upper, HALF_LON, WLON)
                tip_out[1] = lines(lower, HALF_LON, WLON)
                copies.append(remote(tip_out.at[0], tip_back.at[0], sems, last_lat, (0, 1)))
                copies.append(remote(tip_out.at[1], tip_back.at[1], sems, lat_wins, (1, 1)))
        if t == last_lat:
            rows_out[b] = lines(lower, 0, WLON)
            copies.append(
                remote(rows_out.at[b], rows_back.at[b], sems, lat_wins + 1 + b, (1, 0))
            )
        for copy in copies:
            copy.start()
        return copies

    for load in loads[5:]:
        load.wait()
    ready = set()

    def fetch(group):
        needed = set()
        for t, b in group:
            needed |= {t} if b == last_lon else set()
            if t == last_lat:
                needed |= {lat_wins, lat_wins + 1} if b == last_lon else {lat_wins}
        for which in sorted(needed - ready):
            ahead[which].wait_recv()
        ready.update(needed)
        for t, b in group:
            gather(t, b)

    def attention(group):
        first = slot_of[group[0]]
        taken = wins[first : first + len(group)].reshape(len(group) * tokens, width)
        normed = norm_rows(taken)
        packed = jnp.dot(normed, w_qkv[:, : 2 * width], preferred_element_type=jnp.float32)
        packed = packed.astype(jnp.bfloat16)
        yield
        contexts = []
        for place, (t, b) in enumerate(group):
            part = slice(place * tokens, (place + 1) * tokens)
            work = attend_window(
                heads, normed[part], packed[part, :width], packed[part, width:],
                region_row(t, b), bias, step, t * heads * step, w_vt, turned.at[first + place],
            )
            for context in work:
                yield
            contexts.append(context)
        context = jnp.concatenate(contexts, axis=0)
        projected = jnp.dot(context, w_proj[...], preferred_element_type=jnp.float32)
        projected = projected.astype(jnp.bfloat16).astype(jnp.float32)
        residual = (taken + projected).astype(jnp.bfloat16).astype(jnp.float32)
        yield residual, norm_rows(residual)

    returns = []
    behind = None
    for group in [*groups, None]:
        works = []
        if group is not None:
            fetch(group)
            works.append((attention(group), 2 + len(group) * (width // LANES + 1)))
        if behind is not None:
            works.append((feed_forward(*passed, w_fc1, w_fc2), w_fc1.shape[1] // CHUNK + 1))
        values = weave(*works)
        if behind is not None:
            summed = values[-1]
            first = slot_of[behind[0]]
            wins[first : first + len(behind)] = summed.reshape(len(behind), tokens, width)
            for place, (t, b) in enumerate(behind):
                returns += send_back(summed, t, b, place * tokens)
        behind, passed = group, values[0]

    for copy in ahead:
        copy.wait_send()
    for copy in returns:
        copy.wait()

    for level in range(levels):
        for r in range(lat_rows):
            if r < HALF_LAT:
                at = level * HALF_LAT + r
                kept = [rows_back[b, at * WLON : (at + 1) * WLON] for b in range(lon_wins)]
                halo = tip_back[1, at * HALF_LON : (at + 1) * HALF_LON]
            else:
                t, a = divmod(r - HALF_LAT, WLAT)
                at = level * WLAT + a
                kept = [wins[slot_of[t, b], at * WLON : (at + 1) * WLON] for b in range(lon_wins)]
                if t < last_lat:
                    halo = cols_back[t, at * HALF_LON : (at + 1) * HALF_LON]
                else:
                    at = level * HALF_LAT + a
                    halo = tip_back[0, at * HALF_LON : (at + 1) * HALF_LON]
            kept[-1] = kept[-1][:HALF_LON]
            line = jnp.concatenate([halo, *kept], axis=0) if r < HALF_LAT else jnp.concatenate(
                [halo.astype(jnp.float32), *kept], axis=0
            )
            out[(level + WZ // 2) % levels, r] = line.astype(jnp.bfloat16)


def local(fields, region_ids, bias_index, earth_bias, w_qkv, w_proj, w_fc1, w_fc2):
    levels, lat_rows, lon_cols, width = fields.shape
    lat_wins, lon_wins = lat_rows // WLAT, lon_cols // WLON
    tokens = levels * WLAT * WLON
    bands, positions, heads = earth_bias.shape
    rest = tokens - LANES
    spare = -(-HALF_LON // 8) * 8
    step = tokens + 2 * rest + 8
    pieces = -(-positions // LO)
    whole, _, _, tiles = table_rows(bands * heads, pieces)
    count = lat_wins * lon_wins
    lines = levels * WLAT
    bf16, f32 = jnp.bfloat16, jnp.float32
    weights = (w_qkv, w_proj, w_fc1, w_fc2)
    near = pl.BlockSpec(memory_space=pltpu.VMEM)
    far = pl.BlockSpec(memory_space=pltpu.HBM)
    dma = pltpu.SemaphoreType.DMA
    scratch = [
        pltpu.VMEM(bias_index.shape, jnp.int32),
        pltpu.VMEM((lat_rows, levels, lon_cols), jnp.int32),
        pltpu.VMEM((bands, heads, positions), bf16),
        *[pltpu.VMEM(weight.shape, bf16) for weight in weights],
        pltpu.VMEM((width, width), bf16),
        pltpu.VMEM((tokens, LANES), jnp.int32),
        pltpu.VMEM((rest, LANES), jnp.int32),
        pltpu.VMEM((rest * rest // LANES, LANES), jnp.int32),
        pltpu.VMEM((pieces * whole + 8 * tiles, LO), bf16),
        pltpu.VMEM((bands * heads * step, LANES), f32),
        pltpu.VMEM(fields.shape, bf16),
        pltpu.VMEM((levels, lat_rows, spare, width), bf16),
        pltpu.VMEM((levels, HALF_LAT, lon_cols, width), bf16),
        pltpu.VMEM((levels, HALF_LAT, spare, width), bf16),
        pltpu.VMEM((count, tokens, width), f32),
        pltpu.VMEM((count, width, LANES), f32),
        pltpu.VMEM((max(lat_wins - 1, 1), lines * HALF_LON, width), bf16),
        pltpu.VMEM((max(lat_wins - 1, 1), lines * HALF_LON, width), bf16),
        pltpu.VMEM((2, lines // 2 * HALF_LON, width), bf16),
        pltpu.VMEM((2, lines // 2 * HALF_LON, width), bf16),
        pltpu.VMEM((lon_wins, lines // 2 * WLON, width), bf16),
        pltpu.VMEM((lon_wins, lines // 2 * WLON, width), bf16),
        dma((8,)),
        dma((lat_wins + 2,)),
        dma((lat_wins + 2,)),
        dma((lat_wins + 1 + lon_wins,)),
        dma((lat_wins + 1 + lon_wins,)),
    ]
    return pl.pallas_call(
        functools.partial(layer_kernel, heads, step),
        out_shape=pltpu.VMEM(fields.shape, bf16),
        in_specs=[far] * 8,
        out_specs=near,
        scratch_shapes=scratch,
        compiler_params=pltpu.CompilerParams(
            vmem_limit_bytes=GRANT, collective_id=0, has_side_effects=True
        ),
        cost_estimate=pl.CostEstimate(
            flops=2 * count * tokens * sum(weight.size for weight in weights),
            bytes_accessed=fields.size * 4 + earth_bias.size * 20,
            transcendentals=count * heads * tokens * tokens,
        ),
        name="layer",
    )(
        bias_index, region_ids.transpose(1, 0, 2), fields, earth_bias.transpose(0, 2, 1), *weights
    )


def solution(mesh):
    return jax.shard_map(
        local,
        mesh=mesh,
        in_specs=(
            P("ens", "lat", "lon", None),
            P(None, "lat", "lon"),
            P(),
            P("lat", None, None),
            P(),
            P(),
            P(),
            P(),
        ),
        out_specs=P("ens", "lat", "lon", None),
        check_vma=False,
    )
```

```python
import functools
import math

import jax
import jax.numpy as jnp
from jax import lax
from jax.experimental import pallas as pl
from jax.experimental.pallas import tpu as pltpu
from jax.sharding import PartitionSpec as P

WZ = 2
WLAT = 6
WLON = 12
HALF_LAT = WLAT // 2
HALF_LON = WLON // 2
EPS_NORM = 1e-05
LOG2E = math.log2(math.e)
LO = 256
LANES = 128
AT_ONCE = 4
EARLY = 2
MOST = (2, 1, 2, 2)
HEAD = 0
UNROLL = 8
CHUNK = 256
GRANT = 64000000
NT = (((1,), (1,)), ((), ()))
MESH = pl.DeviceIdType.MESH


def norm_rows(wide):
    average = jnp.mean(wide, axis=-1, keepdims=True)
    centred = wide - average
    spread = jnp.mean(centred * centred, axis=-1, keepdims=True)
    return (centred * lax.rsqrt(spread + EPS_NORM)).astype(jnp.bfloat16)


def table_rows(count, pieces):
    whole = count // 8 * 8
    left = count - whole
    fold = 8 // left if left else 1
    tiles = -(-pieces // fold) if left else 0
    return whole, left, fold, tiles


def build_table(earth, table):
    bands, heads, positions = earth.shape
    pieces = -(-positions // LO)
    whole, left, fold, tiles = table_rows(bands * heads, pieces)
    ends = []
    for piece in range(pieces):
        start = piece * LO
        size = min(LO, positions - start)
        parts = [earth[band, :, start : start + size].astype(jnp.float32) for band in range(bands)]
        parts = [jnp.pad(part, ((0, 0), (0, LO - size))) for part in parts]
        rows = jnp.concatenate(parts, axis=0)
        table[piece * whole : (piece + 1) * whole, :] = rows[:whole].astype(jnp.bfloat16)
        ends.append(rows[whole:])
    if left:
        base = pieces * whole
        for tile in range(tiles):
            rows = ends[tile * fold : (tile + 1) * fold]
            spare = 8 - left * len(rows)
            if spare:
                rows = [*rows, jnp.zeros((spare, LO), jnp.float32)]
            rows = jnp.concatenate(rows, axis=0).astype(jnp.bfloat16)
            table[base + tile * 8 : base + (tile + 1) * 8, :] = rows


def split_index(index, main_idx, left_idx, right_idx):
    tokens = index.shape[0]
    rest = tokens - LANES
    wide = jnp.pad(index[...], ((0, 0), (0, 2 * LANES - tokens)))
    main_idx[...] = wide[:LANES].T[:tokens]
    left_idx[...] = wide[LANES:, :LANES]
    beside = LANES // rest
    corner = wide[LANES:, LANES:]
    for line in range(rest // beside):
        parts = [corner[line * beside + i : line * beside + i + 1, :rest] for i in range(beside)]
        right_idx[line : line + 1, :] = jnp.concatenate(parts, axis=1)


def fill_bias(main_idx, left_idx, right_idx, table, bias, count, pieces, step, begin, end, unroll):
    tokens = main_idx.shape[0]
    rest = left_idx.shape[0]
    whole, left, fold, tiles = table_rows(count, pieces)
    low = lax.broadcasted_iota(jnp.int32, (LO, LANES), 0).astype(jnp.bfloat16)
    one, zero = jnp.ones((), jnp.bfloat16), jnp.zeros((), jnp.bfloat16)

    def lookup(lines):
        rows = [(line & (LO - 1)).astype(jnp.bfloat16) for line in lines]
        spots = jnp.concatenate([jnp.where(low == row, one, zero) for row in rows], axis=1)
        found = jnp.dot(table[...], spots, preferred_element_type=jnp.float32)
        high = [line // LO for line in lines]
        spans = [slice(i * LANES, (i + 1) * LANES) for i in range(len(lines))]
        total = [found[:whole, span] for span in spans]
        for piece in range(1, pieces):
            for i, span in enumerate(spans):
                here = found[piece * whole : (piece + 1) * whole, span]
                total[i] = jnp.where(high[i] == piece, here, total[i])
        if left:
            base = pieces * whole
            ends = [found[base : base + 8, span] for span in spans]
            for tile in range(1, tiles):
                for i, span in enumerate(spans):
                    here = found[base + tile * 8 : base + (tile + 1) * 8, span]
                    ends[i] = jnp.where(high[i] // fold == tile, here, ends[i])
            for i, end in enumerate(ends):
                picked = end[:left]
                for part in range(1, fold):
                    here = end[part * left : (part + 1) * left]
                    picked = jnp.where(high[i] % fold == part, here, picked)
                total[i] = (total[i], picked)
        else:
            total = [(values, None) for values in total]
        return total

    def keep(place, values):
        bias[pl.ds(place, whole, stride=step), :] = values[0] * LOG2E
        if left:
            bias[pl.ds(place + whole * step, left, stride=step), :] = values[1] * LOG2E

    @pl.loop(begin, end, unroll=math.gcd(end - begin, unroll))
    def _(block):
        rows = main_idx[pl.ds(pl.multiple_of(block * 8, 8), 8), :]
        for start in range(0, 8, AT_ONCE):
            lines = [rows[start + line : start + line + 1] for line in range(AT_ONCE)]
            for line, values in enumerate(lookup(lines)):
                keep(block * 8 + start + line, values)

    if end < tokens // 8:
        return

    for start in range(0, rest, AT_ONCE):
        lines = [left_idx[line : line + 1, :] for line in range(start, min(start + AT_ONCE, rest))]
        for line, values in enumerate(lookup(lines)):
            keep(tokens + start + line, values)
    beside = LANES // rest
    lines = [right_idx[line : line + 1, :] for line in range(rest // beside)]
    for line, values in enumerate(lookup(lines)):
        for i in range(beside):
            turned = [
                part if part is None or i == 0 else pltpu.roll(part, LANES - i * rest, axis=1)
                for part in values
            ]
            keep(tokens + rest + line * beside + i, turned)


def attend_window(heads, normed, query, key, row, bias, step, base, w_vt, turned):
    tokens, width = normed.shape
    dim = width // heads
    per = LANES // dim
    rest = tokens - LANES
    scale = dim ** (-0.5) * LOG2E
    value_t = lax.dot_general(w_vt[...], normed, NT, preferred_element_type=jnp.float32)
    value_t = value_t.astype(jnp.bfloat16)
    row = row.astype(jnp.float32)
    diagonal = lax.broadcasted_iota(jnp.int32, (tokens, tokens), 0) == lax.broadcasted_iota(
        jnp.int32, (tokens, tokens), 1
    )
    col = jnp.sum(jnp.where(diagonal, row, 0.0), axis=1, keepdims=True)
    barred = jnp.where(col == row[:, :LANES], 0.0, -jnp.inf)
    owner = lax.broadcasted_iota(jnp.int32, (LANES, LANES), 1) // dim
    zero = jnp.zeros((), jnp.bfloat16)
    raws = []
    for group in range(width // LANES):
        span = slice(group * LANES, (group + 1) * LANES)
        asked = query[:LANES, span]
        stacked = jnp.concatenate([jnp.where(owner == h, asked, zero) for h in range(per)], axis=0)
        raws.append(
            lax.dot_general(key[:, span], stacked, NT, preferred_element_type=jnp.float32)
        )
    holder = lax.broadcasted_iota(jnp.int32, (rest, width), 1) // dim
    asked = query[LANES:]
    stacked = jnp.concatenate([jnp.where(holder == h, asked, zero) for h in range(heads)], axis=0)
    ends = lax.dot_general(stacked, key, NT, preferred_element_type=jnp.float32)
    for group in range(width // LANES):
        raw = raws[group]
        for h in range(per):
            head = group * per + h
            scores = raw[:, h * LANES : (h + 1) * LANES] * scale
            scores = scores + bias[base + head * step : base + head * step + tokens, :] + barred
            grown = jnp.exp2(scores - jnp.max(scores, axis=0, keepdims=True))
            total = jnp.sum(grown, axis=0, keepdims=True)
            mixed = jnp.dot(
                value_t[head * dim : (head + 1) * dim],
                grown.astype(jnp.bfloat16),
                preferred_element_type=jnp.float32,
            )
            turned[head * dim : (head + 1) * dim, :] = mixed / total
        yield
    scores = ends * scale
    starts = [base + h * step + tokens for h in range(heads)]
    left = jnp.concatenate([bias[start : start + rest, :] for start in starts], axis=0)
    right = jnp.concatenate([bias[start + rest : start + 2 * rest, :] for start in starts], axis=0)
    scores = scores + jnp.concatenate([left, right[:, : tokens - LANES]], axis=1)
    barred = jnp.where(col[LANES:] == row, 0.0, -jnp.inf)
    scores = scores + jnp.concatenate([barred] * heads, axis=0)
    grown = jnp.exp2(scores - jnp.max(scores, axis=1, keepdims=True))
    total = jnp.sum(grown, axis=1, keepdims=True)
    mixed = lax.dot_general(
        grown.astype(jnp.bfloat16), value_t, NT, preferred_element_type=jnp.float32
    )
    mixed = mixed / total
    last = jnp.zeros((rest, width), jnp.float32)
    for h in range(heads):
        last = jnp.where(holder == h, mixed[h * rest : (h + 1) * rest], last)
    yield jnp.concatenate([turned[...].T, last], axis=0).astype(jnp.bfloat16)


def feed_forward(residual, normed, w_fc1, w_fc2):
    hidden = []
    for start in range(0, w_fc1.shape[1], CHUNK):
        grown = jnp.dot(
            normed, w_fc1[:, start : start + CHUNK], preferred_element_type=jnp.float32
        )
        halved = 0.5 * grown * (1.0 + lax.erf(grown * math.sqrt(0.5)))
        hidden.append(halved.astype(jnp.bfloat16))
        yield
    hidden = jnp.concatenate(hidden, axis=1)
    yield residual + jnp.dot(hidden, w_fc2[...], preferred_element_type=jnp.float32)


def weave(*works):
    steps = [count for work, count in works]
    done, values = [0] * len(works), [None] * len(works)
    for _ in range(sum(steps)):
        which = min(
            (i for i in range(len(works)) if done[i] < steps[i]),
            key=lambda i: (done[i] + 0.5) / steps[i],
        )
        values[which] = next(works[which][0])
        done[which] += 1
    return values


def window_groups(lat_wins, lon_wins):
    last_lat, last_lon = lat_wins - 1, lon_wins - 1
    inner = [(t, b) for b in range(last_lon) for t in range(last_lat)]
    kinds = [
        inner[:HEAD],
        [(t, last_lon) for t in range(lat_wins)],
        [(last_lat, b) for b in range(last_lon)],
        inner[HEAD:],
    ]
    return [
        kind[first : first + most]
        for kind, most in zip(kinds, MOST)
        for first in range(0, len(kind), most)
    ]


def layer_kernel(
    heads, step, index_far, regions_far, fields, earth_far, qkv_far, proj_far, fc1_far,
    fc2_far, out, index, regions, earth, w_qkv, w_proj, w_fc1, w_fc2, w_vt, main_idx, left_idx,
    right_idx, table, bias, own, cols, rows, corner,
    wins, turned, cols_out, cols_back, tip_out, tip_back, rows_out, rows_back,
    load_sems, there_sems, here_sems, send_sems, take_sems,
):
    levels, lat_rows, lon_cols, width = own.shape
    lat_wins, lon_wins = lat_rows // WLAT, lon_cols // WLON
    last_lat, last_lon = lat_wins - 1, lon_wins - 1
    spare = corner.shape[2]
    tokens = wins.shape[1]
    dim = width // heads
    groups = window_groups(lat_wins, lon_wins)
    order = sum(groups, [])
    slot_of = {window: slot for slot, window in enumerate(order)}

    me_lat, me_lon = lax.axis_index("lat"), lax.axis_index("lon")
    lats, lons = lax.axis_size("lat"), lax.axis_size("lon")

    def device(lat, lon):
        return {
            "lat": lax.rem(me_lat + lat + lats, lats), "lon": lax.rem(me_lon + lon + lons, lons)
        }

    barrier = pltpu.get_barrier_semaphore()
    around = [(0, -1), (0, 1), (-1, 0), (1, 0), (-1, -1), (1, 1)]
    for where in around:
        pl.semaphore_signal(barrier, inc=1, device_id=device(*where), device_id_type=MESH)

    far = (earth_far, index_far, regions_far, fields, qkv_far, proj_far, fc1_far, fc2_far)
    near = (earth, index, regions, own, w_qkv, w_proj, w_fc1, w_fc2)
    loads = [
        pltpu.make_async_copy(source, target, load_sems.at[i])
        for i, (source, target) in enumerate(zip(far, near))
    ]
    for load in loads:
        load.start()

    def remote(source, target, sems, place, where):
        return pltpu.make_async_remote_copy(
            src_ref=source, dst_ref=target, send_sem=sems[0].at[place], recv_sem=sems[1].at[place],
            device_id=device(*where), device_id_type=MESH,
        )

    ahead = []
    for t in range(lat_wins):
        low, high = t * WLAT + HALF_LAT, min((t + 1) * WLAT + HALF_LAT, lat_rows)
        ahead.append(
            remote(
                fields.at[:, low:high, :spare, :], cols.at[:, low:high], (there_sems, here_sems),
                t, (0, -1),
            )
        )
    tops = fields.at[:, :HALF_LAT]
    ahead.append(remote(tops, rows, (there_sems, here_sems), lat_wins, (-1, 0)))
    edge = fields.at[:, :HALF_LAT, :spare, :]
    ahead.append(remote(edge, corner, (there_sems, here_sems), lat_wins + 1, (-1, -1)))

    loads[0].wait()
    build_table(earth, table)
    loads[1].wait()
    split_index(index, main_idx, left_idx, right_idx)
    loads[4].wait()
    turn = w_qkv[:, 2 * width :].astype(jnp.float32).T
    w_vt[...] = turn.astype(jnp.bfloat16)

    blocks = tokens // 8
    look = functools.partial(
        fill_bias, main_idx, left_idx, right_idx, table, bias, earth.shape[0] * heads,
        -(-earth.shape[2] // LO), step,
    )
    look(0, EARLY, EARLY)
    pl.semaphore_wait(barrier, len(around))
    for copy in ahead[:last_lat]:
        copy.start()
    ahead[-1].start()
    ahead[last_lat].start()
    ahead[lat_wins].start()
    look(EARLY, blocks, UNROLL)

    loads[2].wait()
    loads[3].wait()

    def gather(t, b):
        span = slice(b * WLON, (b + 1) * WLON)
        for level in range(levels):
            source = (level + WZ // 2) % levels
            for a in range(t * WLAT, (t + 1) * WLAT):
                away = a - (lat_rows - HALF_LAT)
                kept = own[source, a + HALF_LAT] if away < 0 else rows[source, away]
                line = kept.astype(jnp.float32)[HALF_LON:]
                if b == last_lon:
                    halo = cols[source, a + HALF_LAT] if away < 0 else corner[source, away]
                    line = jnp.concatenate([line, halo.astype(jnp.float32)[:HALF_LON]], axis=0)
                place = (level * WLAT + a % WLAT) * WLON
                wins[slot_of[t, b], place : place + WLON, :] = line[span]

    def region_row(t, b):
        span = slice(b * WLON, (b + 1) * WLON)
        parts = [
            regions[t * WLAT + a, level : level + 1, span]
            for level in range(levels)
            for a in range(WLAT)
        ]
        return jnp.concatenate(parts, axis=1)

    def send_back(result, t, b, base):
        copies = []
        count = levels * WLAT

        def lines(chosen, start, stop):
            parts = [result[base + k * WLON + start : base + k * WLON + stop] for k in chosen]
            return jnp.concatenate(parts, axis=0).astype(jnp.bfloat16)

        upper = [k for k in range(count) if k % WLAT < HALF_LAT]
        lower = [k for k in range(count) if k % WLAT >= HALF_LAT]
        sems = (send_sems, take_sems)
        if b == last_lon:
            if t < last_lat:
                cols_out[t] = lines(range(count), HALF_LON, WLON)
                copies.append(remote(cols_out.at[t], cols_back.at[t], sems, t, (0, 1)))
            else:
                tip_out[0] = lines(upper, HALF_LON, WLON)
                tip_out[1] = lines(lower, HALF_LON, WLON)
                copies.append(remote(tip_out.at[0], tip_back.at[0], sems, last_lat, (0, 1)))
                copies.append(remote(tip_out.at[1], tip_back.at[1], sems, lat_wins, (1, 1)))
        if t == last_lat:
            rows_out[b] = lines(lower, 0, WLON)
            copies.append(
                remote(rows_out.at[b], rows_back.at[b], sems, lat_wins + 1 + b, (1, 0))
            )
        for copy in copies:
            copy.start()
        return copies

    for load in loads[5:]:
        load.wait()
    ready = set()

    def fetch(group):
        needed = set()
        for t, b in group:
            needed |= {t} if b == last_lon else set()
            if t == last_lat:
                needed |= {lat_wins, lat_wins + 1} if b == last_lon else {lat_wins}
        for which in sorted(needed - ready):
            ahead[which].wait_recv()
        ready.update(needed)
        for t, b in group:
            gather(t, b)

    def attention(group):
        first = slot_of[group[0]]
        taken = wins[first : first + len(group)].reshape(len(group) * tokens, width)
        normed = norm_rows(taken)
        packed = jnp.dot(normed, w_qkv[:, : 2 * width], preferred_element_type=jnp.float32)
        packed = packed.astype(jnp.bfloat16)
        yield
        works = []
        for place, (t, b) in enumerate(group):
            part = slice(place * tokens, (place + 1) * tokens)
            works.append(
                attend_window(
                    heads, normed[part], packed[part, :width], packed[part, width:],
                    region_row(t, b), bias, step, t * heads * step, w_vt, turned.at[first + place],
                )
            )
        for _ in range(width // LANES + 1):
            contexts = []
            for work in works:
                contexts.append(next(work))
                yield
        context = jnp.concatenate(contexts, axis=0)
        projected = jnp.dot(context, w_proj[...], preferred_element_type=jnp.float32)
        projected = projected.astype(jnp.bfloat16).astype(jnp.float32)
        residual = (taken + projected).astype(jnp.bfloat16).astype(jnp.float32)
        yield residual, norm_rows(residual)

    returns = []
    behind = None
    for group in [*groups, None]:
        works = []
        if group is not None:
            fetch(group)
            works.append((attention(group), 2 + len(group) * (width // LANES + 1)))
        if behind is not None:
            works.append((feed_forward(*passed, w_fc1, w_fc2), w_fc1.shape[1] // CHUNK + 1))
        values = weave(*works)
        if behind is not None:
            summed = values[-1]
            first = slot_of[behind[0]]
            wins[first : first + len(behind)] = summed.reshape(len(behind), tokens, width)
            for place, (t, b) in enumerate(behind):
                returns += send_back(summed, t, b, place * tokens)
        behind, passed = group, values[0]

    for copy in ahead:
        copy.wait_send()
    for copy in returns:
        copy.wait()

    for level in range(levels):
        for r in range(lat_rows):
            if r < HALF_LAT:
                at = level * HALF_LAT + r
                kept = [rows_back[b, at * WLON : (at + 1) * WLON] for b in range(lon_wins)]
                halo = tip_back[1, at * HALF_LON : (at + 1) * HALF_LON]
            else:
                t, a = divmod(r - HALF_LAT, WLAT)
                at = level * WLAT + a
                kept = [wins[slot_of[t, b], at * WLON : (at + 1) * WLON] for b in range(lon_wins)]
                if t < last_lat:
                    halo = cols_back[t, at * HALF_LON : (at + 1) * HALF_LON]
                else:
                    at = level * HALF_LAT + a
                    halo = tip_back[0, at * HALF_LON : (at + 1) * HALF_LON]
            kept[-1] = kept[-1][:HALF_LON]
            line = jnp.concatenate([halo, *kept], axis=0) if r < HALF_LAT else jnp.concatenate(
                [halo.astype(jnp.float32), *kept], axis=0
            )
            out[(level + WZ // 2) % levels, r] = line.astype(jnp.bfloat16)


def local(fields, region_ids, bias_index, earth_bias, w_qkv, w_proj, w_fc1, w_fc2):
    levels, lat_rows, lon_cols, width = fields.shape
    lat_wins, lon_wins = lat_rows // WLAT, lon_cols // WLON
    tokens = levels * WLAT * WLON
    bands, positions, heads = earth_bias.shape
    rest = tokens - LANES
    spare = -(-HALF_LON // 8) * 8
    step = tokens + 2 * rest + 8
    pieces = -(-positions // LO)
    whole, _, _, tiles = table_rows(bands * heads, pieces)
    count = lat_wins * lon_wins
    lines = levels * WLAT
    bf16, f32 = jnp.bfloat16, jnp.float32
    weights = (w_qkv, w_proj, w_fc1, w_fc2)
    near = pl.BlockSpec(memory_space=pltpu.VMEM)
    far = pl.BlockSpec(memory_space=pltpu.HBM)
    dma = pltpu.SemaphoreType.DMA
    scratch = [
        pltpu.VMEM(bias_index.shape, jnp.int32),
        pltpu.VMEM((lat_rows, levels, lon_cols), jnp.int32),
        pltpu.VMEM((bands, heads, positions), bf16),
        *[pltpu.VMEM(weight.shape, bf16) for weight in weights],
        pltpu.VMEM((width, width), bf16),
        pltpu.VMEM((tokens, LANES), jnp.int32),
        pltpu.VMEM((rest, LANES), jnp.int32),
        pltpu.VMEM((rest * rest // LANES, LANES), jnp.int32),
        pltpu.VMEM((pieces * whole + 8 * tiles, LO), bf16),
        pltpu.VMEM((bands * heads * step, LANES), f32),
        pltpu.VMEM(fields.shape, bf16),
        pltpu.VMEM((levels, lat_rows, spare, width), bf16),
        pltpu.VMEM((levels, HALF_LAT, lon_cols, width), bf16),
        pltpu.VMEM((levels, HALF_LAT, spare, width), bf16),
        pltpu.VMEM((count, tokens, width), f32),
        pltpu.VMEM((count, width, LANES), f32),
        pltpu.VMEM((max(lat_wins - 1, 1), lines * HALF_LON, width), bf16),
        pltpu.VMEM((max(lat_wins - 1, 1), lines * HALF_LON, width), bf16),
        pltpu.VMEM((2, lines // 2 * HALF_LON, width), bf16),
        pltpu.VMEM((2, lines // 2 * HALF_LON, width), bf16),
        pltpu.VMEM((lon_wins, lines // 2 * WLON, width), bf16),
        pltpu.VMEM((lon_wins, lines // 2 * WLON, width), bf16),
        dma((8,)),
        dma((lat_wins + 2,)),
        dma((lat_wins + 2,)),
        dma((lat_wins + 1 + lon_wins,)),
        dma((lat_wins + 1 + lon_wins,)),
    ]
    return pl.pallas_call(
        functools.partial(layer_kernel, heads, step),
        out_shape=pltpu.VMEM(fields.shape, bf16),
        in_specs=[far] * 8,
        out_specs=near,
        scratch_shapes=scratch,
        compiler_params=pltpu.CompilerParams(
            vmem_limit_bytes=GRANT, collective_id=0, has_side_effects=True
        ),
        cost_estimate=pl.CostEstimate(
            flops=2 * count * tokens * sum(weight.size for weight in weights),
            bytes_accessed=fields.size * 4 + earth_bias.size * 20,
            transcendentals=count * heads * tokens * tokens,
        ),
        name="layer",
    )(
        bias_index, region_ids.transpose(1, 0, 2), fields, earth_bias.transpose(0, 2, 1), *weights
    )


def solution(mesh):
    return jax.shard_map(
        local,
        mesh=mesh,
        in_specs=(
            P("ens", "lat", "lon", None),
            P(None, "lat", "lon"),
            P(),
            P("lat", None, None),
            P(),
            P(),
            P(),
            P(),
        ),
        out_specs=P("ens", "lat", "lon", None),
        check_vma=False,
    )
```

```python
import functools
import math

import jax
import jax.numpy as jnp
from jax import lax
from jax.experimental import pallas as pl
from jax.experimental.pallas import tpu as pltpu
from jax.sharding import PartitionSpec as P

WZ = 2
WLAT = 6
WLON = 12
HALF_LAT = WLAT // 2
HALF_LON = WLON // 2
EPS_NORM = 1e-05
LOG2E = math.log2(math.e)
LO = 256
LANES = 128
AT_ONCE = 4
EARLY = 2
MOST = (2, 2, 2, 2)
HEAD = 0
UNROLL = 8
CHUNK = 1536
SOON = True
GRANT = 64000000
NT = (((1,), (1,)), ((), ()))
MESH = pl.DeviceIdType.MESH


def norm_rows(wide):
    average = jnp.mean(wide, axis=-1, keepdims=True)
    centred = wide - average
    spread = jnp.mean(centred * centred, axis=-1, keepdims=True)
    return (centred * lax.rsqrt(spread + EPS_NORM)).astype(jnp.bfloat16)


def table_rows(count, pieces):
    whole = count // 8 * 8
    left = count - whole
    fold = 8 // left if left else 1
    tiles = -(-pieces // fold) if left else 0
    return whole, left, fold, tiles


def build_table(earth, table):
    bands, heads, positions = earth.shape
    pieces = -(-positions // LO)
    whole, left, fold, tiles = table_rows(bands * heads, pieces)
    ends = []
    for piece in range(pieces):
        start = piece * LO
        size = min(LO, positions - start)
        parts = [earth[band, :, start : start + size].astype(jnp.float32) for band in range(bands)]
        parts = [jnp.pad(part, ((0, 0), (0, LO - size))) for part in parts]
        rows = jnp.concatenate(parts, axis=0)
        table[piece * whole : (piece + 1) * whole, :] = rows[:whole].astype(jnp.bfloat16)
        ends.append(rows[whole:])
    if left:
        base = pieces * whole
        for tile in range(tiles):
            rows = ends[tile * fold : (tile + 1) * fold]
            spare = 8 - left * len(rows)
            if spare:
                rows = [*rows, jnp.zeros((spare, LO), jnp.float32)]
            rows = jnp.concatenate(rows, axis=0).astype(jnp.bfloat16)
            table[base + tile * 8 : base + (tile + 1) * 8, :] = rows


def split_index(index, main_idx, left_idx, right_idx):
    tokens = index.shape[0]
    rest = tokens - LANES
    wide = jnp.pad(index[...], ((0, 0), (0, 2 * LANES - tokens)))
    main_idx[...] = wide[:LANES].T[:tokens]
    left_idx[...] = wide[LANES:, :LANES]
    beside = LANES // rest
    corner = wide[LANES:, LANES:]
    for line in range(rest // beside):
        parts = [corner[line * beside + i : line * beside + i + 1, :rest] for i in range(beside)]
        right_idx[line : line + 1, :] = jnp.concatenate(parts, axis=1)


def fill_bias(main_idx, left_idx, right_idx, table, bias, count, pieces, step, begin, end, unroll):
    tokens = main_idx.shape[0]
    rest = left_idx.shape[0]
    whole, left, fold, tiles = table_rows(count, pieces)
    low = lax.broadcasted_iota(jnp.int32, (LO, LANES), 0).astype(jnp.bfloat16)
    one, zero = jnp.ones((), jnp.bfloat16), jnp.zeros((), jnp.bfloat16)

    def lookup(lines):
        rows = [(line & (LO - 1)).astype(jnp.bfloat16) for line in lines]
        spots = jnp.concatenate([jnp.where(low == row, one, zero) for row in rows], axis=1)
        found = jnp.dot(table[...], spots, preferred_element_type=jnp.float32)
        high = [line // LO for line in lines]
        spans = [slice(i * LANES, (i + 1) * LANES) for i in range(len(lines))]
        total = [found[:whole, span] for span in spans]
        for piece in range(1, pieces):
            for i, span in enumerate(spans):
                here = found[piece * whole : (piece + 1) * whole, span]
                total[i] = jnp.where(high[i] == piece, here, total[i])
        if left:
            base = pieces * whole
            ends = [found[base : base + 8, span] for span in spans]
            for tile in range(1, tiles):
                for i, span in enumerate(spans):
                    here = found[base + tile * 8 : base + (tile + 1) * 8, span]
                    ends[i] = jnp.where(high[i] // fold == tile, here, ends[i])
            for i, end in enumerate(ends):
                picked = end[:left]
                for part in range(1, fold):
                    here = end[part * left : (part + 1) * left]
                    picked = jnp.where(high[i] % fold == part, here, picked)
                total[i] = (total[i], picked)
        else:
            total = [(values, None) for values in total]
        return total

    def keep(place, values):
        bias[pl.ds(place, whole, stride=step), :] = values[0] * LOG2E
        if left:
            bias[pl.ds(place + whole * step, left, stride=step), :] = values[1] * LOG2E

    @pl.loop(begin, end, unroll=math.gcd(end - begin, unroll))
    def _(block):
        rows = main_idx[pl.ds(pl.multiple_of(block * 8, 8), 8), :]
        for start in range(0, 8, AT_ONCE):
            lines = [rows[start + line : start + line + 1] for line in range(AT_ONCE)]
            for line, values in enumerate(lookup(lines)):
                keep(block * 8 + start + line, values)

    if end < tokens // 8:
        return

    for start in range(0, rest, AT_ONCE):
        lines = [left_idx[line : line + 1, :] for line in range(start, min(start + AT_ONCE, rest))]
        for line, values in enumerate(lookup(lines)):
            keep(tokens + start + line, values)
    beside = LANES // rest
    lines = [right_idx[line : line + 1, :] for line in range(rest // beside)]
    for line, values in enumerate(lookup(lines)):
        for i in range(beside):
            turned = [
                part if part is None or i == 0 else pltpu.roll(part, LANES - i * rest, axis=1)
                for part in values
            ]
            keep(tokens + rest + line * beside + i, turned)


def attend_window(heads, normed, query, key, row, bias, step, base, w_vt, turned):
    tokens, width = normed.shape
    dim = width // heads
    per = LANES // dim
    rest = tokens - LANES
    scale = dim ** (-0.5) * LOG2E
    value_t = lax.dot_general(w_vt[...], normed, NT, preferred_element_type=jnp.float32)
    value_t = value_t.astype(jnp.bfloat16)
    row = row.astype(jnp.float32)
    diagonal = lax.broadcasted_iota(jnp.int32, (tokens, tokens), 0) == lax.broadcasted_iota(
        jnp.int32, (tokens, tokens), 1
    )
    col = jnp.sum(jnp.where(diagonal, row, 0.0), axis=1, keepdims=True)
    barred = jnp.where(col == row[:, :LANES], 0.0, -jnp.inf)
    owner = lax.broadcasted_iota(jnp.int32, (LANES, LANES), 1) // dim
    zero = jnp.zeros((), jnp.bfloat16)
    raws = []
    for group in range(width // LANES):
        span = slice(group * LANES, (group + 1) * LANES)
        asked = query[:LANES, span]
        stacked = jnp.concatenate([jnp.where(owner == h, asked, zero) for h in range(per)], axis=0)
        raws.append(
            lax.dot_general(key[:, span], stacked, NT, preferred_element_type=jnp.float32)
        )
    holder = lax.broadcasted_iota(jnp.int32, (rest, width), 1) // dim
    asked = query[LANES:]
    stacked = jnp.concatenate([jnp.where(holder == h, asked, zero) for h in range(heads)], axis=0)
    ends = lax.dot_general(stacked, key, NT, preferred_element_type=jnp.float32)
    for group in range(width // LANES):
        raw = raws[group]
        for h in range(per):
            head = group * per + h
            scores = raw[:, h * LANES : (h + 1) * LANES] * scale
            scores = scores + bias[base + head * step : base + head * step + tokens, :] + barred
            grown = jnp.exp2(scores - jnp.max(scores, axis=0, keepdims=True))
            total = jnp.sum(grown, axis=0, keepdims=True)
            mixed = jnp.dot(
                value_t[head * dim : (head + 1) * dim],
                grown.astype(jnp.bfloat16),
                preferred_element_type=jnp.float32,
            )
            turned[head * dim : (head + 1) * dim, :] = mixed / total
        yield
    scores = ends * scale
    starts = [base + h * step + tokens for h in range(heads)]
    left = jnp.concatenate([bias[start : start + rest, :] for start in starts], axis=0)
    right = jnp.concatenate([bias[start + rest : start + 2 * rest, :] for start in starts], axis=0)
    scores = scores + jnp.concatenate([left, right[:, : tokens - LANES]], axis=1)
    barred = jnp.where(col[LANES:] == row, 0.0, -jnp.inf)
    scores = scores + jnp.concatenate([barred] * heads, axis=0)
    grown = jnp.exp2(scores - jnp.max(scores, axis=1, keepdims=True))
    total = jnp.sum(grown, axis=1, keepdims=True)
    mixed = lax.dot_general(
        grown.astype(jnp.bfloat16), value_t, NT, preferred_element_type=jnp.float32
    )
    mixed = mixed / total
    last = jnp.zeros((rest, width), jnp.float32)
    for h in range(heads):
        last = jnp.where(holder == h, mixed[h * rest : (h + 1) * rest], last)
    yield jnp.concatenate([turned[...].T, last], axis=0).astype(jnp.bfloat16)


def feed_forward(residual, normed, w_fc1, w_fc2):
    hidden = []
    for start in range(0, w_fc1.shape[1], CHUNK):
        grown = jnp.dot(
            normed, w_fc1[:, start : start + CHUNK], preferred_element_type=jnp.float32
        )
        halved = 0.5 * grown * (1.0 + lax.erf(grown * math.sqrt(0.5)))
        hidden.append(halved.astype(jnp.bfloat16))
        yield
    hidden = jnp.concatenate(hidden, axis=1)
    yield residual + jnp.dot(hidden, w_fc2[...], preferred_element_type=jnp.float32)


def weave(*works):
    steps = [count for work, count in works]
    done, values = [0] * len(works), [None] * len(works)
    for _ in range(sum(steps)):
        which = min(
            (i for i in range(len(works)) if done[i] < steps[i]),
            key=lambda i: (done[i] + 0.5) / steps[i],
        )
        values[which] = next(works[which][0])
        done[which] += 1
    return values


def window_groups(lat_wins, lon_wins):
    last_lat, last_lon = lat_wins - 1, lon_wins - 1
    inner = [(t, b) for b in range(last_lon) for t in range(last_lat)]
    kinds = [
        inner[:HEAD],
        [(t, last_lon) for t in range(lat_wins)],
        [(last_lat, b) for b in range(last_lon)],
        inner[HEAD:],
    ]
    return [
        kind[first : first + most]
        for kind, most in zip(kinds, MOST)
        for first in range(0, len(kind), most)
    ]


def layer_kernel(
    heads, step, index_far, regions_far, fields, earth_far, qkv_far, proj_far, fc1_far,
    fc2_far, out, index, regions, earth, w_qkv, w_proj, w_fc1, w_fc2, w_vt, main_idx, left_idx,
    right_idx, table, bias, own, cols, rows, corner,
    wins, turned, cols_out, cols_back, tip_out, tip_back, rows_out, rows_back,
    load_sems, there_sems, here_sems, send_sems, take_sems,
):
    levels, lat_rows, lon_cols, width = own.shape
    lat_wins, lon_wins = lat_rows // WLAT, lon_cols // WLON
    last_lat, last_lon = lat_wins - 1, lon_wins - 1
    spare = corner.shape[2]
    tokens = wins.shape[1]
    dim = width // heads
    groups = window_groups(lat_wins, lon_wins)
    order = sum(groups, [])
    slot_of = {window: slot for slot, window in enumerate(order)}

    me_lat, me_lon = lax.axis_index("lat"), lax.axis_index("lon")
    lats, lons = lax.axis_size("lat"), lax.axis_size("lon")

    def device(lat, lon):
        return {
            "lat": lax.rem(me_lat + lat + lats, lats), "lon": lax.rem(me_lon + lon + lons, lons)
        }

    barrier = pltpu.get_barrier_semaphore()
    around = [(0, -1), (0, 1), (-1, 0), (1, 0), (-1, -1), (1, 1)]
    for where in around:
        pl.semaphore_signal(barrier, inc=1, device_id=device(*where), device_id_type=MESH)

    far = (earth_far, index_far, regions_far, fields, qkv_far, proj_far, fc1_far, fc2_far)
    near = (earth, index, regions, own, w_qkv, w_proj, w_fc1, w_fc2)
    loads = [
        pltpu.make_async_copy(source, target, load_sems.at[i])
        for i, (source, target) in enumerate(zip(far, near))
    ]
    for load in loads:
        load.start()

    def remote(source, target, sems, place, where):
        return pltpu.make_async_remote_copy(
            src_ref=source, dst_ref=target, send_sem=sems[0].at[place], recv_sem=sems[1].at[place],
            device_id=device(*where), device_id_type=MESH,
        )

    ahead = []
    for t in range(lat_wins):
        low, high = t * WLAT + HALF_LAT, min((t + 1) * WLAT + HALF_LAT, lat_rows)
        ahead.append(
            remote(
                fields.at[:, low:high, :spare, :], cols.at[:, low:high], (there_sems, here_sems),
                t, (0, -1),
            )
        )
    tops = fields.at[:, :HALF_LAT]
    ahead.append(remote(tops, rows, (there_sems, here_sems), lat_wins, (-1, 0)))
    edge = fields.at[:, :HALF_LAT, :spare, :]
    ahead.append(remote(edge, corner, (there_sems, here_sems), lat_wins + 1, (-1, -1)))

    loads[0].wait()
    build_table(earth, table)
    loads[1].wait()
    split_index(index, main_idx, left_idx, right_idx)
    loads[4].wait()
    turn = w_qkv[:, 2 * width :].astype(jnp.float32).T
    w_vt[...] = turn.astype(jnp.bfloat16)

    blocks = tokens // 8
    look = functools.partial(
        fill_bias, main_idx, left_idx, right_idx, table, bias, earth.shape[0] * heads,
        -(-earth.shape[2] // LO), step,
    )
    look(0, EARLY, EARLY)
    pl.semaphore_wait(barrier, len(around))
    for copy in ahead[:last_lat]:
        copy.start()
    ahead[-1].start()
    ahead[last_lat].start()
    ahead[lat_wins].start()
    look(EARLY, blocks, UNROLL)

    loads[2].wait()
    loads[3].wait()

    def gather(t, b):
        span = slice(b * WLON, (b + 1) * WLON)
        for level in range(levels):
            source = (level + WZ // 2) % levels
            for a in range(t * WLAT, (t + 1) * WLAT):
                away = a - (lat_rows - HALF_LAT)
                kept = own[source, a + HALF_LAT] if away < 0 else rows[source, away]
                line = kept.astype(jnp.float32)[HALF_LON:]
                if b == last_lon:
                    halo = cols[source, a + HALF_LAT] if away < 0 else corner[source, away]
                    line = jnp.concatenate([line, halo.astype(jnp.float32)[:HALF_LON]], axis=0)
                place = (level * WLAT + a % WLAT) * WLON
                wins[slot_of[t, b], place : place + WLON, :] = line[span]

    def region_row(t, b):
        span = slice(b * WLON, (b + 1) * WLON)
        parts = [
            regions[t * WLAT + a, level : level + 1, span]
            for level in range(levels)
            for a in range(WLAT)
        ]
        return jnp.concatenate(parts, axis=1)

    def send_back(result, t, b, base):
        copies = []
        count = levels * WLAT

        def lines(chosen, start, stop):
            parts = [result[base + k * WLON + start : base + k * WLON + stop] for k in chosen]
            return jnp.concatenate(parts, axis=0).astype(jnp.bfloat16)

        upper = [k for k in range(count) if k % WLAT < HALF_LAT]
        lower = [k for k in range(count) if k % WLAT >= HALF_LAT]
        sems = (send_sems, take_sems)
        if b == last_lon:
            if t < last_lat:
                cols_out[t] = lines(range(count), HALF_LON, WLON)
                copies.append(remote(cols_out.at[t], cols_back.at[t], sems, t, (0, 1)))
            else:
                tip_out[0] = lines(upper, HALF_LON, WLON)
                tip_out[1] = lines(lower, HALF_LON, WLON)
                copies.append(remote(tip_out.at[0], tip_back.at[0], sems, last_lat, (0, 1)))
                copies.append(remote(tip_out.at[1], tip_back.at[1], sems, lat_wins, (1, 1)))
        if t == last_lat:
            rows_out[b] = lines(lower, 0, WLON)
            copies.append(
                remote(rows_out.at[b], rows_back.at[b], sems, lat_wins + 1 + b, (1, 0))
            )
        for copy in copies:
            copy.start()
        return copies

    for load in loads[5:]:
        load.wait()
    ready = set()

    def fetch(group):
        needed = set()
        for t, b in group:
            needed |= {t} if b == last_lon else set()
            if t == last_lat:
                needed |= {lat_wins, lat_wins + 1} if b == last_lon else {lat_wins}
        for which in sorted(needed - ready):
            ahead[which].wait_recv()
        ready.update(needed)
        for t, b in group:
            gather(t, b)

    def attention(group):
        first = slot_of[group[0]]
        taken = wins[first : first + len(group)].reshape(len(group) * tokens, width)
        normed = norm_rows(taken)
        packed = jnp.dot(normed, w_qkv[:, : 2 * width], preferred_element_type=jnp.float32)
        packed = packed.astype(jnp.bfloat16)
        yield
        works = []
        for place, (t, b) in enumerate(group):
            part = slice(place * tokens, (place + 1) * tokens)
            works.append(
                attend_window(
                    heads, normed[part], packed[part, :width], packed[part, width:],
                    region_row(t, b), bias, step, t * heads * step, w_vt, turned.at[first + place],
                )
            )
        for _ in range(width // LANES + 1):
            contexts = []
            for work in works:
                contexts.append(next(work))
                yield
        context = jnp.concatenate(contexts, axis=0)
        projected = jnp.dot(context, w_proj[...], preferred_element_type=jnp.float32)
        projected = projected.astype(jnp.bfloat16).astype(jnp.float32)
        residual = (taken + projected).astype(jnp.bfloat16).astype(jnp.float32)
        yield residual, norm_rows(residual)

    returns = []

    def finish(group, summed):
        first = slot_of[group[0]]
        wins[first : first + len(group)] = summed.reshape(len(group), tokens, width)
        copies = []
        for place, (t, b) in enumerate(group):
            copies += send_back(summed, t, b, place * tokens)
        return copies

    def front(group):
        return attention(group), 2 + len(group) * (width // LANES + 1)

    def back(passed):
        return feed_forward(*passed, w_fc1, w_fc2), w_fc1.shape[1] // CHUNK + 1

    behind = None
    for group in groups:
        fetch(group)
        if behind is None:
            (passed,) = weave(front(group))
        else:
            ahead_of, summed = weave(front(group), back(passed))
            returns += finish(behind, summed)
            passed = ahead_of
        behind = group
        if SOON and group[0][1] == last_lon:
            (summed,) = weave(back(passed))
            returns += finish(group, summed)
            behind = None
    if behind is not None:
        (summed,) = weave(back(passed))
        returns += finish(behind, summed)

    for copy in ahead:
        copy.wait_send()
    for copy in returns:
        copy.wait()

    for level in range(levels):
        for r in range(lat_rows):
            if r < HALF_LAT:
                at = level * HALF_LAT + r
                kept = [rows_back[b, at * WLON : (at + 1) * WLON] for b in range(lon_wins)]
                halo = tip_back[1, at * HALF_LON : (at + 1) * HALF_LON]
            else:
                t, a = divmod(r - HALF_LAT, WLAT)
                at = level * WLAT + a
                kept = [wins[slot_of[t, b], at * WLON : (at + 1) * WLON] for b in range(lon_wins)]
                if t < last_lat:
                    halo = cols_back[t, at * HALF_LON : (at + 1) * HALF_LON]
                else:
                    at = level * HALF_LAT + a
                    halo = tip_back[0, at * HALF_LON : (at + 1) * HALF_LON]
            kept[-1] = kept[-1][:HALF_LON]
            line = jnp.concatenate([halo, *kept], axis=0) if r < HALF_LAT else jnp.concatenate(
                [halo.astype(jnp.float32), *kept], axis=0
            )
            out[(level + WZ // 2) % levels, r] = line.astype(jnp.bfloat16)


def local(fields, region_ids, bias_index, earth_bias, w_qkv, w_proj, w_fc1, w_fc2):
    levels, lat_rows, lon_cols, width = fields.shape
    lat_wins, lon_wins = lat_rows // WLAT, lon_cols // WLON
    tokens = levels * WLAT * WLON
    bands, positions, heads = earth_bias.shape
    rest = tokens - LANES
    spare = -(-HALF_LON // 8) * 8
    step = tokens + 2 * rest + 8
    pieces = -(-positions // LO)
    whole, _, _, tiles = table_rows(bands * heads, pieces)
    count = lat_wins * lon_wins
    lines = levels * WLAT
    bf16, f32 = jnp.bfloat16, jnp.float32
    weights = (w_qkv, w_proj, w_fc1, w_fc2)
    near = pl.BlockSpec(memory_space=pltpu.VMEM)
    far = pl.BlockSpec(memory_space=pltpu.HBM)
    dma = pltpu.SemaphoreType.DMA
    scratch = [
        pltpu.VMEM(bias_index.shape, jnp.int32),
        pltpu.VMEM((lat_rows, levels, lon_cols), jnp.int32),
        pltpu.VMEM((bands, heads, positions), bf16),
        *[pltpu.VMEM(weight.shape, bf16) for weight in weights],
        pltpu.VMEM((width, width), bf16),
        pltpu.VMEM((tokens, LANES), jnp.int32),
        pltpu.VMEM((rest, LANES), jnp.int32),
        pltpu.VMEM((rest * rest // LANES, LANES), jnp.int32),
        pltpu.VMEM((pieces * whole + 8 * tiles, LO), bf16),
        pltpu.VMEM((bands * heads * step, LANES), f32),
        pltpu.VMEM(fields.shape, bf16),
        pltpu.VMEM((levels, lat_rows, spare, width), bf16),
        pltpu.VMEM((levels, HALF_LAT, lon_cols, width), bf16),
        pltpu.VMEM((levels, HALF_LAT, spare, width), bf16),
        pltpu.VMEM((count, tokens, width), f32),
        pltpu.VMEM((count, width, LANES), f32),
        pltpu.VMEM((max(lat_wins - 1, 1), lines * HALF_LON, width), bf16),
        pltpu.VMEM((max(lat_wins - 1, 1), lines * HALF_LON, width), bf16),
        pltpu.VMEM((2, lines // 2 * HALF_LON, width), bf16),
        pltpu.VMEM((2, lines // 2 * HALF_LON, width), bf16),
        pltpu.VMEM((lon_wins, lines // 2 * WLON, width), bf16),
        pltpu.VMEM((lon_wins, lines // 2 * WLON, width), bf16),
        dma((8,)),
        dma((lat_wins + 2,)),
        dma((lat_wins + 2,)),
        dma((lat_wins + 1 + lon_wins,)),
        dma((lat_wins + 1 + lon_wins,)),
    ]
    return pl.pallas_call(
        functools.partial(layer_kernel, heads, step),
        out_shape=pltpu.VMEM(fields.shape, bf16),
        in_specs=[far] * 8,
        out_specs=near,
        scratch_shapes=scratch,
        compiler_params=pltpu.CompilerParams(
            vmem_limit_bytes=GRANT, collective_id=0, has_side_effects=True
        ),
        cost_estimate=pl.CostEstimate(
            flops=2 * count * tokens * sum(weight.size for weight in weights),
            bytes_accessed=fields.size * 4 + earth_bias.size * 20,
            transcendentals=count * heads * tokens * tokens,
        ),
        name="layer",
    )(
        bias_index, region_ids.transpose(1, 0, 2), fields, earth_bias.transpose(0, 2, 1), *weights
    )


def solution(mesh):
    return jax.shard_map(
        local,
        mesh=mesh,
        in_specs=(
            P("ens", "lat", "lon", None),
            P(None, "lat", "lon"),
            P(),
            P("lat", None, None),
            P(),
            P(),
            P(),
            P(),
        ),
        out_specs=P("ens", "lat", "lon", None),
        check_vma=False,
    )
```
